128 devices in a mesh: cols: 32 (over x, z, y_lo), trc: 4 (over y_hi, core).
Axes of the slice: x: 4, y: 4 (y_hi: 2, y_lo: 2; y = y_hi * 2 + y_lo), z: 4, core: 2. Of those that a mesh axis runs over, the one named last changes fastest.
Arguments:
- tracers_src: bfloat16 [28, 127, 65536], P(None, None, ('cols', 'trc')), may hold values from -1 to 2
- layer_dp: float32 [127, 65536], P(None, ('cols', 'trc')), may hold values from 0.3 to 3
- cut_frac: float32 [71, 65536], P(None, ('cols', 'trc')), may hold values from 0.05 to 0.95
- level_bounds: int32 [2, 72, 65536], P(None, None, ('cols', 'trc')), may hold values from 0 to 126, as said below
Outputs:
- remapped_tracers: bfloat16 [28, 72, 65536], P('trc', None, 'cols')
- burden: float32 [28], P('trc')
The draws below stay inside these ranges and needn't reach their ends.
Inputs may be any that keep to these rules, and one draw needn't show every extreme that they name: level_bounds[0, 0, c] = 0, level_bounds[1, 71, c] = 126, level_bounds[1, t, c] = level_bounds[0, t + 1, c], and level_bounds[0, t, c] rises strictly with t in every column.
All inputs are finite; a program needn't handle non-finite values.
Results may differ from the reference program's by a relative error of at most 0.0005.
Values may be sent and summed in bfloat16 or wider, within the bound.
No kernel may reach another device: no remote copies, remote signals or barrier semaphores. Data moves between devices by JAX's collectives and lax.ppermute only.
A program may use at most 64 MiB of HBM per device.

```python
import math
import jax
import jax.numpy as jnp
from jax import lax

TR = 28
KS = 127
KT = 72
COLS = 65536


def draw_level_bounds(key, part):
    random_scores = jax.random.randint(key, (KS - 2, COLS), 0, 1 << 20)
    random_scores = random_scores * (KS - 2) + lax.broadcasted_iota(jnp.int32, (KS - 2, COLS), 0)
    ordering = jnp.argsort(random_scores, axis=0)
    picked = jnp.sort(ordering[:KT - 1], axis=0).astype(jnp.int32) + 1
    first_layer = jnp.concatenate([jnp.zeros((1, COLS), jnp.int32), picked], axis=0)
    last_layer = jnp.concatenate([picked, jnp.full((1, COLS), KS - 1, jnp.int32)], axis=0)
    return jnp.stack([first_layer, last_layer]).astype(jnp.int32)


def levels(rng, extent, pieces, least, high):
    gain, own = 1.0, jax.random.fold_in(rng, 6)
    for dim, shards_of in pieces:
        heights = jnp.exp(jax.random.uniform(jax.random.fold_in(own, dim), (shards_of,), jnp.float32, least / len(pieces), high / len(pieces)))
        gain = gain * jnp.repeat(heights, extent[dim] // shards_of).reshape([-1 if axis == dim else 1 for axis in range(len(extent))])
    return gain


def setup_inputs(seed: int = 0) -> dict:
    streams_of = jax.random.split(jax.random.key(seed), 5)
    tracers_src = jnp.clip(-1.0 + 3.0 * jax.random.uniform(streams_of[0], (TR, KS, COLS), jnp.float32) ** levels(streams_of[0], (TR, KS, COLS), ((2, 128),), -0.2, 0.2), -1.0, 2.0).astype(jnp.bfloat16)
    layer_dp = jnp.clip(jnp.exp(math.log(3.0) - 2.3025851 * jax.random.uniform(streams_of[1], (KS, COLS), jnp.float32) ** levels(streams_of[1], (KS, COLS), ((1, 128),), -0.2, 0.2)), 0.3, 3.0)
    cut_frac = jnp.clip(0.05 + 0.9 * jax.random.uniform(streams_of[2], (KT - 1, COLS), jnp.float32) ** levels(streams_of[2], (KT - 1, COLS), ((1, 128),), -0.2, 0.2), 0.05, 0.95)
    level_bounds = draw_level_bounds(jax.random.fold_in(streams_of[4], 71), 0)
    return {"tracers_src": tracers_src, "layer_dp": layer_dp, "cut_frac": cut_frac, "level_bounds": level_bounds}


def remap_block(tracers, layer_dp, cut_frac, bounds):
    columns = layer_dp.shape[1]
    tracer_count = tracers.shape[0]
    src_edges = jnp.concatenate([jnp.zeros((1, columns), jnp.float32), jnp.cumsum(layer_dp, axis=0)], axis=0)
    inner_first = bounds[0][1:].astype(jnp.int32)
    base_edge = jnp.take_along_axis(src_edges, inner_first, axis=0)
    chosen_dp = jnp.take_along_axis(layer_dp, inner_first, axis=0)
    inner_edges = base_edge + cut_frac * chosen_dp
    targets = jnp.concatenate([jnp.zeros((1, columns), jnp.float32), inner_edges, src_edges[-1:]], axis=0)
    layer_mass = tracers.astype(jnp.float32) * layer_dp[None]
    cum_mass = jnp.concatenate([jnp.zeros((tracer_count, 1, columns), jnp.float32), jnp.cumsum(layer_mass, axis=1)], axis=1)
    index_all = jnp.broadcast_to(inner_first[None], (tracer_count,) + inner_first.shape)
    inner_mass = jnp.take_along_axis(cum_mass, index_all, axis=1) + cut_frac[None] * jnp.take_along_axis(layer_mass, index_all, axis=1)
    edge_mass = jnp.concatenate([jnp.zeros((tracer_count, 1, columns), jnp.float32), inner_mass, cum_mass[:, -1:]], axis=1)
    remapped = edge_mass[:, 1:] - edge_mass[:, :-1]
    return remapped, targets[1:] - targets[:-1], cum_mass[:, -1]


def reference(tracers_src, layer_dp, cut_frac, level_bounds):
    block_cols = math.gcd(COLS, 512)
    block_count = COLS // block_cols

    def remap_one(block_index):
        offset = block_index * block_cols
        return remap_block(
            lax.dynamic_slice_in_dim(tracers_src, offset, block_cols, 2),
            lax.dynamic_slice_in_dim(layer_dp, offset, block_cols, 1),
            lax.dynamic_slice_in_dim(cut_frac, offset, block_cols, 1),
            lax.dynamic_slice_in_dim(level_bounds, offset, block_cols, 2))

    remapped, target_dp, column_mass = lax.map(remap_one, jnp.arange(block_count, dtype=jnp.int32))
    remapped = jnp.moveaxis(remapped, 0, 2).reshape(TR, KT, COLS)
    target_dp = jnp.moveaxis(target_dp, 0, 1).reshape(KT, COLS)
    column_mass = jnp.moveaxis(column_mass, 0, 1).reshape(TR, COLS)
    position = lax.broadcasted_iota(jnp.int32, (COLS,), 0)
    cell_area = 1.0 + 2.0 * position.astype(jnp.float32) / COLS
    norm_scale = 1.0 / (COLS * KS)
    burden = jnp.sum(column_mass * cell_area[None], axis=1) * norm_scale
    positive = jnp.maximum(remapped / target_dp[None], 0.0)
    burden_after = jnp.sum(positive * target_dp[None] * cell_area[None, None], axis=(1, 2)) * norm_scale
    fix_ratio = burden / burden_after
    return (positive * fix_ratio[:, None, None]).astype(jnp.bfloat16), burden
```

```python
import functools
import jax, jax.numpy as jnp
from jax import lax
from jax.experimental import pallas as pl
from jax.experimental.pallas import tpu as pltpu
from jax.sharding import Mesh
from jax.sharding import PartitionSpec as P

TRC = ("trc_0", "trc_1")
COLS = ("cols_0", "cols_1", "cols_2")
COLS_TRC = ("cols_0", "cols_1", "cols_2", "trc_0", "trc_1")
F32=jnp.float32; BF=jnp.bfloat16; I32=jnp.int32

def gath(x, idx):
    return jnp.take_along_axis(x, idx, axis=0, mode="promise_in_bounds")

def remap_kernel(meta_ref, tr_ref, dp_ref, cf_ref, lb_ref, o0, o1, o2, o3, s0, s1, s2, s3, part_ref,
                 tri, idx_s, over_s, hi_s, psi_s, inv_s, dbuf, fbuf, *, total_cols, cb0):
    r = pl.program_id(1)
    g = meta_ref[0]
    row8 = lax.broadcasted_iota(I32, (8, 128), 0)
    KT, NV = 72, 9

    def compact(gv, e_masks):
        y = []
        for v in range(15):
            ix = idx_s[8*v:8*v+8, :]
            ov = over_s[8*v:8*v+8, :] != 0
            y.append(jnp.where(ov, gath(gv[v+1], ix), gath(gv[v], ix)))
        out = []
        for o in range(NV):
            m0, m1, m2 = (e_masks[k][8*o:8*o+8, :] != 0 for k in range(3))
            a0 = jnp.where(m0, y[o+1], y[o]); a1 = jnp.where(m0, y[o+3], y[o+2])
            a2 = jnp.where(m0, y[o+5], y[o+4]); a3 = y[o+6]
            c0 = jnp.where(m1, a1, a0); c1 = jnp.where(m1, a3, a2)
            out.append(jnp.where(m2, c1, c0))
        return out

    def diffs(e, total):
        rolled = [pltpu.roll(x, 7, 0) for x in e]
        tb = jnp.broadcast_to(total, (8, 128))
        out = []
        for o in range(NV):
            nxt = rolled[o+1] if o + 1 < NV else tb
            out.append(jnp.where(row8 == 7, nxt, rolled[o]) - e[o])
        return out

    def cums(mass):
        hi = mass.astype(BF)
        mid = (mass - hi.astype(F32)).astype(BF)
        x = jnp.concatenate([hi, mid], axis=0)
        return jnp.dot(tri[...], x, preferred_element_type=F32)

    @pl.when(r == 0)
    def _():
        rr = lax.broadcasted_iota(I32, (128, 256), 0)
        cc = lax.broadcasted_iota(I32, (128, 256), 1) & 127
        tri[...] = (cc < rr).astype(F32).astype(BF)
        b = lb_ref[0]
        jrow = lax.broadcasted_iota(I32, (KT, 128), 0)
        d = b - jrow
        H = d >> 3
        dl = d & 7
        hi_s[0] = H & 1
        hi_s[1] = H & 2
        hi_s[2] = H & 4
        f = jnp.concatenate([jnp.zeros((1, 128), F32), cf_ref[...]], axis=0)
        dbuf[0:8, :] = jnp.zeros((8, 128), I32)
        fbuf[0:8, :] = jnp.zeros((8, 128), F32)
        for v in range(16):
            dv = jnp.zeros((8, 128), I32); fv = jnp.zeros((8, 128), F32)
            for h in range(7):
                o = v - h
                if 0 <= o < NV:
                    sl = slice(8*o, 8*o+8)
                    m = H[sl] == h
                    dv = jnp.where(m, dl[sl], dv)
                    fv = jnp.where(m, f[sl], fv)
            dbuf[8+8*v:16+8*v, :] = dv
            fbuf[8+8*v:16+8*v, :] = fv
            t = row8 + dv
            idx_s[8*v:8*v+8, :] = t & 7
            over_s[8*v:8*v+8, :] = t >> 3
        phi = jnp.zeros((128, 128), F32)
        for k in range(8):
            phi = phi + jnp.where(dbuf[8-k:136-k, :] == k, fbuf[8-k:136-k, :], 0.0)
        srow = lax.broadcasted_iota(I32, (128, 128), 0)
        dpz = jnp.where(srow < 127, dp_ref[...], 0.0)
        psi = phi * dpz
        psi_s[0] = dpz
        psi_s[1] = psi
        c = cums(dpz)
        gg = c + psi
        e = compact([gg[8*v:8*v+8] for v in range(16)], hi_s)
        td = diffs(e, c[127:128])
        for o in range(NV):
            inv_s[8*o:8*o+8, :] = 1.0 / td[o]

    pos_col = meta_ref[1] + (pl.program_id(0) + cb0) * 128 + lax.broadcasted_iota(I32, (1, 128), 1)
    area = 1.0 + 2.0 * pos_col.astype(F32) / total_cols
    last = lax.broadcasted_iota(I32, (128, 128), 0) < 127
    outs = (o0, o1, o2, o3)
    scs = (s0, s1, s2, s3)
    for pair in range(2):
        trs = [jnp.where(last, tr_ref[g ^ (2*pair+i), 0].astype(F32), 0.0) for i in range(2)]
        dpz, psi = psi_s[0], psi_s[1]
        mass = jnp.concatenate([t * dpz for t in trs], axis=1)
        c = cums(mass)
        for i in range(2):
            ci = c[:, 128*i:128*i+128]
            gg = ci + psi * trs[i]
            e = compact([gg[8*v:8*v+8] for v in range(16)], hi_s)
            total = ci[127:128]
            rem = [jnp.maximum(x, 0.0) for x in diffs(e, total)]
            s = rem[0]
            for o in range(1, NV): s = s + rem[o]
            pos = [rem[o] * inv_s[8*o:8*o+8, :] for o in range(NV)]
            mx = pos[0]
            for o in range(1, NV): mx = jnp.maximum(mx, pos[o])
            mx = jnp.max(mx, axis=0, keepdims=True)
            rs = 65535.0 / jnp.maximum(mx, 1e-33)
            code = [((x * rs + 0.5).astype(I32) - 32768) for x in pos]
            outs[2*pair+i][0] = jnp.concatenate(code, axis=0).astype(jnp.int16)
            scs[2*pair+i][0] = mx
            grp = g ^ (2*pair+i)
            part_ref[0, 0, pl.ds(grp, 1), :] = total * area
            part_ref[0, 0, pl.ds(4 + grp, 1), :] = jnp.sum(s, axis=0, keepdims=True) * area

def remap(meta, tr, dp, cf, lb, total_cols, cb0, ncb):
    TRn, KS, C = tr.shape
    KT = lb.shape[1]
    tr4 = tr.reshape(4, TRn // 4, KS, C)
    R = TRn // 4
    col = lambda c, r, m: c + cb0
    gs = pltpu.PrefetchScalarGridSpec(
        num_scalar_prefetch=1, grid=(ncb, R),
        in_specs=[pl.BlockSpec((4, 1, 128, 128), lambda c, r, m: (0, r, 0, c + cb0)),
                  pl.BlockSpec((128, 128), lambda c, r, m: (0, c + cb0)),
                  pl.BlockSpec((KT - 1, 128), lambda c, r, m: (0, c + cb0)),
                  pl.BlockSpec((1, KT, 128), lambda c, r, m: (0, 0, c + cb0))],
        out_specs=[pl.BlockSpec((1, KT, 128), lambda c, r, m: (r, 0, c))] * 4
        + [pl.BlockSpec((1, 1, 128), lambda c, r, m: (r, 0, c))] * 4
        + [pl.BlockSpec((1, 1, 8, 128), lambda c, r, m: (c, r, 0, 0))],
        scratch_shapes=[pltpu.VMEM((128, 256), BF), pltpu.VMEM((128, 128), I32), pltpu.VMEM((128, 128), I32),
                        pltpu.VMEM((3, KT, 128), I32), pltpu.VMEM((2, 128, 128), F32), pltpu.VMEM((KT, 128), F32),
                        pltpu.VMEM((136, 128), I32), pltpu.VMEM((136, 128), F32)])
    return pl.pallas_call(
        functools.partial(remap_kernel, total_cols=total_cols, cb0=cb0),
        grid_spec=gs,
        out_shape=[jax.ShapeDtypeStruct((R, KT, 128 * ncb), jnp.int16)] * 4
        + [jax.ShapeDtypeStruct((R, 1, 128 * ncb), F32)] * 4
        + [jax.ShapeDtypeStruct((ncb, R, 8, 128), F32)],
        name="remap",
    )(meta, tr4, dp, cf, lb)


def finish_kernel(meta_ref, c0, c1, c2, c3, s0, s1, s2, s3, rat_ref, out_ref):
    step = pl.program_id(0)
    for i, (c, s) in enumerate(((c0, s0), (c1, s1), (c2, s2), (c3, s3))):
        @pl.when(step == i)
        def _():
            for r in range(out_ref.shape[0]):
                gain = s[r] * rat_ref[r]
                v = c[r].astype(I32).astype(F32) + 32768.0
                out_ref[r] = (v * gain).astype(BF)


def finish(meta, codes, scales, ratio):
    R, KT, C = codes[0].shape
    full = [pl.BlockSpec(x.shape, lambda s, m: (0, 0, 0)) for x in codes + scales]
    gs = pltpu.PrefetchScalarGridSpec(
        num_scalar_prefetch=1, grid=(4,),
        in_specs=full + [pl.BlockSpec(memory_space=pltpu.SMEM)],
        out_specs=pl.BlockSpec((R, KT, C), lambda s, m: (0, 0, m[0] ^ s)))
    return pl.pallas_call(
        finish_kernel, grid_spec=gs, out_shape=jax.ShapeDtypeStruct((R, KT, 4 * C), BF),
        name="finish")(meta, *codes, *scales, ratio)


def per_device(tracers_src, layer_dp, cut_frac, level_bounds):
    groups = lax.axis_size(TRC)
    col_dev = layer_dp.shape[1]
    total_cols = col_dev * lax.axis_size(COLS) * groups
    norm_scale = 1.0 / (total_cols * layer_dp.shape[0])
    me = lax.axis_index(TRC)
    start_col = (lax.axis_index(COLS) * groups + me) * col_dev
    meta = jnp.stack([me, start_col]).astype(I32)
    res = remap(meta, tracers_src, layer_dp, cut_frac, level_bounds, total_cols, 0, 4)
    codes, scales, part = list(res[:4]), list(res[4:8]), res[8]
    for i in range(1, 4):
        pairs = [(j, j ^ i) for j in range(4)]
        codes[i] = lax.ppermute(codes[i], TRC, pairs)
        scales[i] = lax.ppermute(scales[i], TRC, pairs)
    sums = jnp.sum(part, axis=(0, 3))
    per = sums.shape[0]
    wide = jnp.pad(sums.reshape(1, per * 8), ((0, 0), (0, 128 - per * 8)))
    wide = lax.all_to_all(jnp.broadcast_to(wide, (16, 128)), ("cols_0", "cols_1"), 0, 0, tiled=True).sum(0)
    mine = wide[:per * 8].reshape(per, 2, groups).transpose(2, 1, 0).reshape(1, groups, 2 * per)
    mine = jnp.broadcast_to(mine, (2, groups, 2 * per)).reshape(2 * groups, 2 * per)
    mine = jnp.pad(mine, ((0, 0), (0, 128 - 2 * per)))
    mine = lax.all_to_all(mine, ("cols_2", "trc_0", "trc_1"), 0, 0, tiled=True).sum(0)
    before, after = mine[:per], mine[per:2 * per]
    burden = before * norm_scale
    ratio = burden / (after * norm_scale) / 65535.0
    return (finish(meta, codes, scales, ratio), burden)


def solution(mesh):
    split = Mesh(
        mesh.devices.reshape(4, 4, 2, 2, 2), ("cols_0", "cols_1", "cols_2", "trc_0", "trc_1")
    )
    return jax.shard_map(
        per_device,
        mesh=split,
        in_specs=(
            P(None, None, COLS_TRC),
            P(None, COLS_TRC),
            P(None, COLS_TRC),
            P(None, None, COLS_TRC),
        ),
        out_specs=(P(TRC, None, COLS), P(TRC)),
        check_vma=False,
    )
```

```python
import functools
import jax
import jax.numpy as jnp
from jax import lax
from jax.experimental import pallas as pl
from jax.experimental.pallas import tpu as pltpu
from jax.sharding import Mesh
from jax.sharding import PartitionSpec as P

TRC = ("trc_0", "trc_1")
COLS = ("cols_0", "cols_1", "cols_2")
COLS_TRC = ("cols_0", "cols_1", "cols_2", "trc_0", "trc_1")
F32, BF, I32 = jnp.float32, jnp.bfloat16, jnp.int32
LANES, TILES, OUT = 128, 16, 9

SUBLANE_GATHER = lax.GatherDimensionNumbers(
    offset_dims=(), collapsed_slice_dims=(0,), start_index_map=(0,),
    operand_batching_dims=(1,), start_indices_batching_dims=(1,))


def pick(x, index):
    return lax.gather(x, index[..., None], SUBLANE_GATHER, slice_sizes=(1, 1),
                      mode=lax.GatherScatterMode.PROMISE_IN_BOUNDS)


def tile(x, v):
    return x[8 * v:8 * v + 8]


LEVELS, EXTRA = 72, 8
CHUNKS = (5, 2)


def remap_kernel(first, size, total_cols, tr_ref, *refs):
    if first == 0:
        dp_ref, cf_ref, lb_ref, o0, o1, o2, o3, sum_ref, idx_s, over_s, bit_s, dp_s, psi_s, inv_s, dbuf, fbuf = refs[:16]
        tri, part_s, top_s, fin_s = refs[16:]
    else:
        sum_in, idx_s, over_s, bit_s, dp_s, psi_s, inv_s, o0, o1, o2, o3, sum_ref, tri, part_s, top_s, fin_s = refs
    r = pl.program_id(0)
    groups = lax.axis_size(TRC)
    me = lax.axis_index(TRC)
    cols = tr_ref.shape[3]
    start = (lax.axis_index(COLS) * groups + me) * cols
    row8 = lax.broadcasted_iota(I32, (8, LANES), 0)

    def cums(mass):
        hi = mass.astype(BF)
        mid = (mass - hi.astype(F32)).astype(BF)
        return jnp.dot(tri[...], jnp.concatenate([hi, mid], axis=0), preferred_element_type=F32)

    def edge_differences(cum, extra, cb):
        n = len(cum)
        point = [tile(cum[i], 0) + tile(extra[i], 0) for i in range(n)]
        low = [[None] * 15 for _ in range(n)]
        edge = [[None] * OUT for _ in range(n)]
        roll = [[None] * (OUT + 1) for _ in range(n)]
        diff = [[None] * OUT for _ in range(n)]
        for v in range(15):
            ix = idx_s[cb, 8 * v:8 * v + 8, :]
            ov = over_s[cb, 8 * v:8 * v + 8, :] != 0
            for i in range(n):
                nxt = tile(cum[i], v + 1) + tile(extra[i], v + 1)
                low[i][v] = jnp.where(ov, pick(nxt, ix), pick(point[i], ix))
                point[i] = nxt
            o = v - 6
            if o >= 0:
                m0, m1, m2 = (bit_s[cb, k, 8 * o:8 * o + 8, :] != 0 for k in range(3))
                for i in range(n):
                    y = low[i]
                    a0 = jnp.where(m0, y[o + 1], y[o])
                    a1 = jnp.where(m0, y[o + 3], y[o + 2])
                    a2 = jnp.where(m0, y[o + 5], y[o + 4])
                    c0 = jnp.where(m1, a1, a0)
                    c1 = jnp.where(m1, y[o + 6], a2)
                    edge[i][o] = jnp.where(m2, c1, c0)
                    roll[i][o] = pltpu.roll(edge[i][o], 7, 0)
                    if o > 0:
                        diff[i][o - 1] = jnp.where(row8 == 7, roll[i][o], roll[i][o - 1]) - edge[i][o - 1]
        for i in range(n):
            total = jnp.broadcast_to(cum[i][127:128], (8, LANES))
            diff[i][OUT - 1] = jnp.where(row8 == 7, total, roll[i][OUT - 1]) - edge[i][OUT - 1]
        return diff

    @pl.when(r == 0)
    def _():
        rr = lax.broadcasted_iota(I32, (LANES, 2 * LANES), 0)
        cc = lax.broadcasted_iota(I32, (LANES, 2 * LANES), 1) & (LANES - 1)
        tri[...] = (cc < rr).astype(F32).astype(BF)
        if first:
            return
        dbuf[0:8, :] = jnp.zeros((8, LANES), I32)
        fbuf[0:8, :] = jnp.zeros((8, LANES), F32)

        def prepare(cb, carry):
            at = pl.ds(pl.multiple_of(cb * LANES, LANES), LANES)
            d = lb_ref[0, :, at] - lax.broadcasted_iota(I32, (8 * OUT, LANES), 0)
            high, lowbits = d >> 3, d & 7
            for k in range(3):
                bit_s[cb, k] = high & (1 << k)
            f = jnp.concatenate([jnp.zeros((1, LANES), F32), cf_ref[:, at]], axis=0)
            for v in range(TILES):
                dv, fv = jnp.zeros((8, LANES), I32), jnp.zeros((8, LANES), F32)
                for h in range(7):
                    if 0 <= v - h < OUT:
                        m = tile(high, v - h) == h
                        dv = jnp.where(m, tile(lowbits, v - h), dv)
                        fv = jnp.where(m, tile(f, v - h), fv)
                dbuf[8 + 8 * v:16 + 8 * v, :] = dv
                fbuf[8 + 8 * v:16 + 8 * v, :] = fv
                t = row8 + dv
                idx_s[cb, 8 * v:8 * v + 8, :] = t & 7
                over_s[cb, 8 * v:8 * v + 8, :] = t >> 3
            phi = jnp.zeros((LANES, LANES), F32)
            for k in range(8):
                phi = phi + jnp.where(dbuf[8 - k:136 - k, :] == k, fbuf[8 - k:136 - k, :], 0.0)
            srow = lax.broadcasted_iota(I32, (LANES, LANES), 0)
            dp = jnp.where(srow < 127, dp_ref[:, at], 0.0)
            psi = phi * dp
            dp_s[cb] = dp
            psi_s[cb] = psi
            (thick,) = edge_differences([cums(dp)], [psi], cb)
            for o in range(OUT):
                inv_s[cb, 8 * o:8 * o + 8, :] = 1.0 / thick[o]
            return carry

        lax.fori_loop(0, cols // LANES, prepare, 0, unroll=4)

    outs = (o0, o1, o2, o3)
    real = lax.broadcasted_iota(I32, (LANES, LANES), 0) < 127

    def block(cb, carry):
        at = pl.ds(pl.multiple_of(cb * LANES, LANES), LANES)
        position = start + cb * LANES + lax.broadcasted_iota(I32, (1, LANES), 1)
        area = 1.0 + 2.0 * position.astype(F32) / total_cols
        dp, psi = dp_s[cb], psi_s[cb]
        befores, afters = [], []
        for pair in range(2):
            tr = [jnp.where(real, tr_ref[me ^ (2 * pair + i), 0, :, at].astype(F32), 0.0) for i in range(2)]
            both = cums(jnp.concatenate([t * dp for t in tr], axis=1))
            cum = [both[:, :LANES], both[:, LANES:]]
            diff = edge_differences(cum, [psi * t for t in tr], cb)
            for i in range(2):
                kept = [jnp.maximum(x, 0.0) for x in diff[i]]
                mass = kept[0]
                for o in range(1, OUT):
                    mass = mass + kept[o]
                mean = [kept[o] * inv_s[cb, 8 * o:8 * o + 8, :] for o in range(OUT)]
                top = mean[0]
                for o in range(1, OUT):
                    top = jnp.maximum(top, mean[o])
                top = jnp.max(top, axis=0, keepdims=True)
                step = jnp.ceil(jnp.log2(jnp.maximum(top, 1e-33)) * 256.0)
                scale = 65534.0 / jnp.exp2(step * (1.0 / 256.0))
                code = [(x * scale + 0.5).astype(I32) - 32768 for x in mean]
                rows = pl.ds(pl.multiple_of(r * LEVELS, 8), LEVELS)
                outs[2 * pair + i][rows, at] = jnp.concatenate(code, axis=0).astype(jnp.int16)
                top_s[2 * pair + i, cb, pl.ds(r, 1), :] = step
                befores.append(cum[i][127:128] * area)
                afters.append(jnp.sum(mass, axis=0, keepdims=True) * area)
        return carry + jnp.concatenate(befores + afters, axis=0)

    part_s[r] = lax.fori_loop(0, cols // LANES, block, jnp.zeros((8, LANES), F32), unroll=4)

    @pl.when(r == size - 1)
    def _():
        for i in range(4):
            tops = jnp.concatenate([top_s[i, c] for c in range(cols // LANES)], axis=1)
            outs[i][size * LEVELS:size * LEVELS + EXTRA, :] = tops.astype(I32).astype(jnp.int16)
        lane = lax.broadcasted_iota(I32, (8, LANES), 1)
        acc = jnp.zeros((8, LANES), F32) if first == 0 else sum_in[...]
        for k in range(size):
            acc = jnp.where(lane == first + k, jnp.sum(part_s[k], axis=1, keepdims=True), acc)
        if first == 0:
            sum_ref[...] = acc
        else:
            fin_s[...] = acc
            rows = jnp.concatenate([fin_s[pl.ds(me ^ t, 1), :] for t in range(4)], axis=0)
            late = jnp.concatenate([fin_s[pl.ds(4 + (me ^ t), 1), :] for t in range(4)], axis=0)
            both = jnp.where(lane[:4] < 64, rows, pltpu.roll(late, 64, 1))
            for k in range(sum_ref.shape[0]):
                sum_ref[k] = both


def remap(first, size, tr, dp, cf, lb, shared, sums, total_cols, copies):
    _, _, cols = tr.shape[1:]
    nb = cols // LANES
    whole = pl.BlockSpec(memory_space=pltpu.VMEM)
    ins = [pl.BlockSpec((4, 1, LANES, cols), lambda r: (0, r + first, 0, 0))]
    outs = [pltpu.VMEM((size * LEVELS + EXTRA, cols), jnp.int16)] * 4
    if first == 0:
        args = (tr, dp, cf, lb)
        ins += [
            pl.BlockSpec((LANES, cols), lambda r: (0, 0)),
            pl.BlockSpec((LEVELS - 1, cols), lambda r: (0, 0)),
            pl.BlockSpec((1, LEVELS, cols), lambda r: (0, 0, 0)),
        ]
        outs += [
            pltpu.VMEM((8, LANES), F32),
            pltpu.VMEM((nb, LANES, LANES), I32),
            pltpu.VMEM((nb, LANES, LANES), I32),
            pltpu.VMEM((nb, 3, LEVELS, LANES), I32),
            pltpu.VMEM((nb, LANES, LANES), F32),
            pltpu.VMEM((nb, LANES, LANES), F32),
            pltpu.VMEM((nb, LEVELS, LANES), F32),
        ]
    else:
        args = (tr, sums, *shared)
        ins += [whole] * 7
        outs += [pltpu.VMEM((copies, 4, LANES), F32)]
    scratch = [pltpu.VMEM((136, LANES), I32), pltpu.VMEM((136, LANES), F32)] if first == 0 else []
    return pl.pallas_call(
        functools.partial(remap_kernel, first, size, total_cols),
        grid=(size,), in_specs=ins, out_specs=[whole] * len(outs), out_shape=outs,
        scratch_shapes=scratch + [
            pltpu.VMEM((LANES, 2 * LANES), BF),
            pltpu.VMEM((size, 8, LANES), F32),
            pltpu.VMEM((4, nb, 8, LANES), F32),
            pltpu.VMEM((8, LANES), F32),
        ],
        cost_estimate=pl.CostEstimate(flops=size * 2_000_000_000, bytes_accessed=size * 1_000_000, transcendentals=0),
        compiler_params=pltpu.CompilerParams(vmem_limit_bytes=16 * 2**20),
        name="remap",
    )(*args)


def finish_kernel(meta_ref, *refs, norm):
    n = len(CHUNKS)
    codes, all_ref, out_ref, burden_ref, gain_s = refs[:4 * n], *refs[4 * n:]
    step = pl.program_id(0)

    @pl.when(step == 0)
    def _():
        burden = jnp.sum(all_ref[...], axis=0, keepdims=True) * norm
        burden_ref[...] = burden
        ratio = burden / pltpu.roll(burden, 64, 1)
        gain_s[...] = jnp.broadcast_to(ratio * (1.0 / 65534.0), gain_s.shape)

    for i in range(4):
        @pl.when(step == i)
        def _():
            at = 0
            for c, size in enumerate(CHUNKS):
                ref = codes[i * n + c]
                tops = jnp.exp2(ref[size * LEVELS:size * LEVELS + EXTRA, :].astype(F32) * (1.0 / 256.0))
                for k in range(size):
                    gain = tops[k:k + 1] * gain_s[0:1, at + k:at + k + 1]
                    code = ref[k * LEVELS:(k + 1) * LEVELS, :].astype(F32)
                    out_ref[at + k] = ((code + 32768.0) * gain).astype(BF)
                at += size


def finish(meta, codes, everyone, norm):
    per, cols = sum(CHUNKS), codes[0].shape[1]
    vmem = pl.BlockSpec(memory_space=pltpu.VMEM)
    return pl.pallas_call(
        functools.partial(finish_kernel, norm=norm),
        grid_spec=pltpu.PrefetchScalarGridSpec(
            num_scalar_prefetch=1, grid=(4,), in_specs=[vmem] * (len(codes) + 1),
            out_specs=[pl.BlockSpec((per, LEVELS, cols), lambda s, m: (0, 0, m[0] ^ s)),
                       pl.BlockSpec((1, LANES), lambda s, m: (0, 0))],
            scratch_shapes=[pltpu.VMEM((8, LANES), F32)]),
        out_shape=[jax.ShapeDtypeStruct((per, LEVELS, 4 * cols), BF),
                   jax.ShapeDtypeStruct((1, LANES), F32)],
        compiler_params=pltpu.CompilerParams(vmem_limit_bytes=16 * 2**20),
        name="finish",
    )(meta, *codes, everyone)


def in_vmem(x):
    return pltpu.with_memory_space_constraint(x, pltpu.VMEM)


def in_hbm(x):
    return pltpu.with_memory_space_constraint(x, pltpu.HBM)


def per_device(tracers_src, layer_dp, cut_frac, level_bounds):
    total_cols = layer_dp.shape[1] * lax.axis_size(COLS_TRC)
    norm = 1.0 / (total_cols * layer_dp.shape[0])
    per = tracers_src.shape[0] // 4
    copies = lax.axis_size(COLS)
    tr = in_hbm(tracers_src.reshape(4, per, *tracers_src.shape[1:]))
    layer_dp, cut_frac, level_bounds = in_hbm(layer_dp), in_hbm(cut_frac), in_hbm(level_bounds)
    codes = [[] for _ in range(4)]
    shared = sums = None
    first = 0
    for size in CHUNKS:
        res = remap(first, size, tr, layer_dp, cut_frac, level_bounds, shared, sums, total_cols, copies)
        sums = res[4]
        if first == 0:
            shared = res[5:]
        codes[0].append(res[0])
        for i in range(1, 4):
            moved = lax.ppermute(res[i], TRC, [(j, j ^ i) for j in range(4)])
            codes[i].append(in_vmem(moved))
        first += size
    everyone = lax.all_to_all(sums.reshape(4 * copies, 1, LANES), COLS_TRC, 0, 0, tiled=True)
    everyone = in_vmem(everyone.reshape(4 * copies, LANES))
    meta = lax.axis_index(TRC).astype(I32).reshape(1)
    result, burden = finish(meta, sum(codes, []), everyone, norm)
    return (result, burden[0, :per])


def solution(mesh):
    split = Mesh(
        mesh.devices.reshape(4, 4, 2, 2, 2), ("cols_0", "cols_1", "cols_2", "trc_0", "trc_1")
    )
    return jax.shard_map(
        per_device,
        mesh=split,
        in_specs=(
            P(None, None, COLS_TRC),
            P(None, COLS_TRC),
            P(None, COLS_TRC),
            P(None, None, COLS_TRC),
        ),
        out_specs=(P(TRC, None, COLS), P(TRC)),
        check_vma=False,
    )
```

```python
import functools
import jax
import jax.numpy as jnp
from jax import lax
from jax.experimental import pallas as pl
from jax.experimental.pallas import tpu as pltpu
from jax.sharding import Mesh
from jax.sharding import PartitionSpec as P

TRC = ("trc_0", "trc_1")
COLS = ("cols_0", "cols_1", "cols_2")
COLS_TRC = ("cols_0", "cols_1", "cols_2", "trc_0", "trc_1")
F32, BF, I32, I16 = jnp.float32, jnp.bfloat16, jnp.int32, jnp.int16
LANES, TILES, OUT = 128, 16, 9
LAYERS, LEVELS, EXTRA = 127, 72, 8
EARLY, LATE = 5, 2

SUBLANE_GATHER = lax.GatherDimensionNumbers(
    offset_dims=(), collapsed_slice_dims=(0,), start_index_map=(0,),
    operand_batching_dims=(1,), start_indices_batching_dims=(1,))


def pick(x, index):
    return lax.gather(x, index[..., None], SUBLANE_GATHER, slice_sizes=(1, 1),
                      mode=lax.GatherScatterMode.PROMISE_IN_BOUNDS)


def tile(x, v):
    return x[8 * v:8 * v + 8]


def row_in_tile():
    return lax.broadcasted_iota(I32, (8, LANES), 0)


def cumulate(tri, mass):
    hi = mass.astype(BF)
    mid = (mass - hi.astype(F32)).astype(BF)
    return jnp.dot(tri[...], jnp.concatenate([hi, mid], axis=0), preferred_element_type=F32)


def edge_differences(cum, extra, cb, idx_s, over_s, one_s, two_s, four_s):
    n = len(cum)
    row8 = row_in_tile()
    y = [[None] * 15 for _ in range(n)]
    z = [[None] * 15 for _ in range(n)]
    w = [[None] * 13 for _ in range(n)]
    edge = [[None] * OUT for _ in range(n)]
    roll = [[None] * OUT for _ in range(n)]
    diff = [[None] * OUT for _ in range(n)]
    point = [tile(cum[i], 0) + extra(i, 0) for i in range(n)]
    for v in range(15):
        ix = idx_s[cb, 8 * v:8 * v + 8, :]
        over = over_s[cb, 8 * v:8 * v + 8, :] != 0
        for i in range(n):
            nxt = tile(cum[i], v + 1) + extra(i, v + 1)
            y[i][v] = jnp.where(over, pick(nxt, ix), pick(point[i], ix))
            point[i] = nxt
        a = v - 1
        if a >= 0:
            m = one_s[cb, 8 * a:8 * a + 8, :] != 0
            for i in range(n):
                z[i][a] = jnp.where(m, y[i][a + 1], y[i][a])
        if v == 14:
            for i in range(n):
                z[i][14] = y[i][14]
        for b in ([v - 3] if v < 14 else [11, 12]):
            if b < 0:
                continue
            m = two_s[cb, 8 * b:8 * b + 8, :] != 0
            for i in range(n):
                w[i][b] = jnp.where(m, z[i][b + 2], z[i][b])
            o = b - 4
            if o < 0:
                continue
            m = four_s[cb, 8 * o:8 * o + 8, :] != 0
            for i in range(n):
                edge[i][o] = jnp.where(m, w[i][o + 4], w[i][o])
                roll[i][o] = pltpu.roll(edge[i][o], 7, 0)
                if o > 0:
                    diff[i][o - 1] = jnp.where(row8 == 7, roll[i][o], roll[i][o - 1]) - edge[i][o - 1]
    for i in range(n):
        total = jnp.broadcast_to(cum[i][LAYERS:LAYERS + 1], (8, LANES))
        diff[i][OUT - 1] = jnp.where(row8 == 7, total, roll[i][OUT - 1]) - edge[i][OUT - 1]
    return diff


def prepare(dp_ref, cf_ref, lb_ref, tri, idx_s, over_s, one_s, two_s, four_s, dp_s, psi_s, inv_s, dbuf, fbuf):
    rr = lax.broadcasted_iota(I32, (LANES, 2 * LANES), 0)
    cc = lax.broadcasted_iota(I32, (LANES, 2 * LANES), 1) & (LANES - 1)
    tri[...] = (cc < rr).astype(F32).astype(BF)
    row8 = row_in_tile()
    zero_i, zero_f = jnp.zeros((8, LANES), I32), jnp.zeros((8, LANES), F32)
    for cb in range(dp_s.shape[0]):
        dbuf[cb, 0:8, :] = zero_i
        fbuf[cb, 0:8, :] = zero_f
        at = slice(cb * LANES, (cb + 1) * LANES)
        d = lb_ref[0, :, at] - lax.broadcasted_iota(I32, (LEVELS, LANES), 0)
        high, low = d >> 3, d & 7
        f = jnp.concatenate([jnp.zeros((1, LANES), F32), cf_ref[:, at]], axis=0)
        for v in range(TILES):
            dv, fv = zero_i, zero_f
            for h in range(7):
                if 0 <= v - h < OUT:
                    m = tile(high, v - h) == h
                    dv = jnp.where(m, tile(low, v - h), dv)
                    fv = jnp.where(m, tile(f, v - h), fv)
            dbuf[cb, 8 + 8 * v:16 + 8 * v, :] = dv
            fbuf[cb, 8 + 8 * v:16 + 8 * v, :] = fv
            t = row8 + dv
            idx_s[cb, 8 * v:8 * v + 8, :] = t & 7
            over_s[cb, 8 * v:8 * v + 8, :] = t >> 3
        for v in range(14):
            bit = zero_i
            for h in (0, 2, 4, 6):
                if 0 <= v - h < OUT:
                    bit = jnp.where(tile(high, v - h) == h + 1, 1, bit)
            one_s[cb, 8 * v:8 * v + 8, :] = bit
        for v in range(13):
            bit = zero_i
            for h in (0, 4):
                if 0 <= v - h < OUT:
                    bit = jnp.where((tile(high, v - h) >> 1) == (h >> 1) + 1, 1, bit)
            two_s[cb, 8 * v:8 * v + 8, :] = bit
        four_s[cb] = high >> 2
        phi = jnp.zeros((LANES, LANES), F32)
        for k in range(8):
            phi = phi + jnp.where(dbuf[cb, 8 - k:136 - k, :] == k, fbuf[cb, 8 - k:136 - k, :], 0.0)
        dp = jnp.concatenate([dp_ref[:, at], jnp.zeros((1, LANES), F32)], axis=0)
        psi = phi * dp
        dp_s[cb] = dp
        psi_s[cb] = psi
        (thick,) = edge_differences(
            [cumulate(tri, dp)], lambda i, v: tile(psi, v), cb, idx_s, over_s, one_s, two_s, four_s)
        for o in range(OUT):
            inv_s[cb, 8 * o:8 * o + 8, :] = 1.0 / thick[o]


def remap_step(r, tr_ref, outs, tabs, extra_s, part_s, top_s, total_cols):
    tri, idx_s, over_s, one_s, two_s, four_s, dp_s, psi_s, inv_s = tabs
    me = lax.axis_index(TRC)
    blocks = dp_s.shape[0]
    start = (lax.axis_index(COLS) * lax.axis_size(TRC) + me) * blocks * LANES
    before, after = [None] * 4, [None] * 4
    for cb in range(blocks):
        at = slice(cb * LANES, (cb + 1) * LANES)
        position = start + cb * LANES + lax.broadcasted_iota(I32, (1, LANES), 1)
        area = 1.0 + 2.0 * position.astype(F32) / total_cols
        for pair in (0, 2):
            mass = []
            for i in range(2):
                t = tr_ref[me ^ (pair + i), :, at].astype(F32)
                t = jnp.concatenate([t, jnp.zeros((1, LANES), F32)], axis=0)
                mass.append(t * dp_s[cb])
                extra_s[cb, pair + i] = t * psi_s[cb]
            both = cumulate(tri, jnp.concatenate(mass, axis=1))
            cum = [both[:, :LANES], both[:, LANES:]]
            diff = edge_differences(
                cum, lambda i, v: extra_s[cb, pair + i, 8 * v:8 * v + 8, :], cb, idx_s, over_s, one_s, two_s, four_s)
            for i in range(2):
                k = pair + i
                kept = [jnp.maximum(x, 0.0) for x in diff[i]]
                mean = [kept[o] * inv_s[cb, 8 * o:8 * o + 8, :] for o in range(OUT)]
                sums, top = kept[0], mean[0]
                for o in range(1, OUT):
                    sums, top = sums + kept[o], jnp.maximum(top, mean[o])
                top = jnp.max(top, axis=0, keepdims=True)
                step = jnp.ceil(jnp.log2(jnp.maximum(top, 1e-33)) * 256.0)
                scale = 65534.0 / jnp.exp2(step * (1.0 / 256.0))
                code = jnp.concatenate([(x * scale + 0.5).astype(I32) for x in mean], axis=0)
                rows = pl.ds(pl.multiple_of(r * LEVELS, 8), LEVELS)
                outs[k][rows, at] = code.astype(I16)
                top_s[k, cb, pl.ds(r, 1), :] = step
                last, area_sum = cum[i][LAYERS:LAYERS + 1] * area, sums * area
                before[k] = last if cb == 0 else before[k] + last
                after[k] = area_sum if cb == 0 else after[k] + area_sum
    part_s[r] = jnp.concatenate(before + [jnp.sum(x, axis=0, keepdims=True) for x in after], axis=0)


def close(first, size, outs, part_s, top_s, acc):
    for i in range(4):
        tops = jnp.concatenate([top_s[i, c] for c in range(top_s.shape[1])], axis=1)
        outs[i][size * LEVELS:size * LEVELS + EXTRA, :] = tops.astype(I32).astype(I16)
    lane = lax.broadcasted_iota(I32, (8, LANES), 1)
    for k in range(size):
        acc = jnp.where(lane == first + k, jnp.sum(part_s[k], axis=1, keepdims=True), acc)
    return acc


def early_kernel(total_cols, tr_hbm, dp_ref, cf_ref, lb_ref, *refs):
    outs, sum_ref, next_ref, tabs = refs[:4], refs[4], refs[5], refs[6:15]
    dbuf, fbuf, held, sems, extra_s, part_s, top_s = refs[15:]
    r = pl.program_id(0)

    def copy(k):
        dst = held.at[k] if k < EARLY else next_ref.at[k - EARLY]
        return pltpu.make_async_copy(tr_hbm.at[:, k], dst, sems.at[k])

    @pl.when(r == 0)
    def _():
        for k in range(EARLY + LATE):
            copy(k).start()
        prepare(dp_ref, cf_ref, lb_ref, *tabs, dbuf, fbuf)

    pltpu.make_async_copy(tr_hbm.at[:, r], held.at[r], sems.at[r]).wait()
    remap_step(r, held.at[r], outs, tabs, extra_s, part_s, top_s, total_cols)

    @pl.when(r == EARLY - 1)
    def _():
        sum_ref[...] = close(0, EARLY, outs, part_s, top_s, jnp.zeros((8, LANES), F32))
        for k in range(EARLY, EARLY + LATE):
            copy(k).wait()


def late_kernel(total_cols, sum_in, tr_ref, *refs):
    tabs, outs, sum_ref = refs[:9], refs[9:13], refs[13]
    extra_s, part_s, top_s, fin_s = refs[14:]
    r = pl.program_id(0)
    remap_step(r, tr_ref.at[r], outs, tabs, extra_s, part_s, top_s, total_cols)

    @pl.when(r == LATE - 1)
    def _():
        me = lax.axis_index(TRC)
        fin_s[...] = close(EARLY, LATE, outs, part_s, top_s, sum_in[...])
        before = jnp.concatenate([fin_s[pl.ds(me ^ t, 1), :] for t in range(4)], axis=0)
        after = jnp.concatenate([fin_s[pl.ds(4 + (me ^ t), 1), :] for t in range(4)], axis=0)
        lane = lax.broadcasted_iota(I32, (4, LANES), 1)
        both = jnp.where(lane < 64, before, pltpu.roll(after, 64, 1))
        for k in range(sum_ref.shape[0]):
            sum_ref[k] = both


WHOLE = pl.BlockSpec(memory_space=pltpu.VMEM)
PARAMS = pltpu.CompilerParams(vmem_limit_bytes=20 * 2**20)


def work(size, cols):
    return [
        pltpu.VMEM((cols // LANES, 4, LANES, LANES), F32),
        pltpu.VMEM((size, 8, LANES), F32),
        pltpu.VMEM((4, cols // LANES, 8, LANES), F32),
    ]


def cost(size):
    return pl.CostEstimate(flops=size * 2_000_000_000, bytes_accessed=size * 1_000_000, transcendentals=0)


def profiles(size, cols):
    return [pltpu.VMEM((size * LEVELS + EXTRA, cols), I16)] * 4


def remap_early(tr, dp, cf, lb, total_cols):
    cols = tr.shape[3]
    nb = cols // LANES
    square = (nb, LANES, LANES)
    outs = profiles(EARLY, cols) + [
        pltpu.VMEM((8, LANES), F32),
        pltpu.VMEM((LATE, 4, LAYERS, cols), BF),
        pltpu.VMEM((LANES, 2 * LANES), BF),
        pltpu.VMEM(square, I32), pltpu.VMEM(square, I32), pltpu.VMEM((nb, 8 * 14, LANES), I32),
        pltpu.VMEM((nb, 8 * 13, LANES), I32), pltpu.VMEM((nb, LEVELS, LANES), I32),
        pltpu.VMEM(square, F32), pltpu.VMEM(square, F32), pltpu.VMEM((nb, LEVELS, LANES), F32),
    ]
    return pl.pallas_call(
        functools.partial(early_kernel, total_cols), grid=(EARLY,),
        in_specs=[
            pl.BlockSpec(memory_space=pltpu.HBM),
            pl.BlockSpec((LAYERS, cols), lambda r: (0, 0)),
            pl.BlockSpec((LEVELS - 1, cols), lambda r: (0, 0)),
            pl.BlockSpec((1, LEVELS, cols), lambda r: (0, 0, 0)),
        ],
        out_specs=[WHOLE] * len(outs), out_shape=outs,
        scratch_shapes=[
            pltpu.VMEM((nb, 136, LANES), I32), pltpu.VMEM((nb, 136, LANES), F32),
            pltpu.VMEM((EARLY, 4, LAYERS, cols), BF), pltpu.SemaphoreType.DMA((EARLY + LATE,)),
        ] + work(EARLY, cols),
        compiler_params=PARAMS, cost_estimate=cost(EARLY), name="remap_early",
    )(tr, dp, cf, lb)


def remap_late(sums, tr, tabs, total_cols, copies):
    cols = tr.shape[3]
    outs = profiles(LATE, cols) + [pltpu.VMEM((copies, 4, LANES), F32)]
    return pl.pallas_call(
        functools.partial(late_kernel, total_cols), grid=(LATE,),
        in_specs=[WHOLE] * 11, out_specs=[WHOLE] * len(outs), out_shape=outs,
        scratch_shapes=work(LATE, cols) + [pltpu.VMEM((8, LANES), F32)],
        compiler_params=PARAMS, cost_estimate=cost(LATE), name="remap_late",
    )(sums, tr, *tabs)


def finish_kernel(meta_ref, *refs, norm):
    codes, (all_ref, out_ref, burden_ref, gain_s) = refs[:8], refs[8:]
    step = pl.program_id(0)
    per = EARLY + LATE

    @pl.when(step == 0)
    def _():
        burden = jnp.sum(all_ref[...], axis=0, keepdims=True) * norm
        burden_ref[...] = burden[0, :per]
        ratio = burden / pltpu.roll(burden, 64, 1)
        gain_s[...] = jnp.broadcast_to(ratio * (1.0 / 65534.0), gain_s.shape)

    for i in range(4):
        @pl.when(step == i)
        def _():
            at = 0
            for ref, size in ((codes[2 * i], EARLY), (codes[2 * i + 1], LATE)):
                tops = jnp.exp2(ref[size * LEVELS:size * LEVELS + EXTRA, :].astype(F32) * (1.0 / 256.0))
                for k in range(size):
                    gain = tops[k:k + 1] * gain_s[0:1, at + k:at + k + 1]
                    code = ref[k * LEVELS:(k + 1) * LEVELS, :].astype(I32) & 65535
                    out_ref[at + k] = (code.astype(F32) * gain).astype(BF)
                at += size


def finish(meta, codes, everyone, norm):
    per, cols = EARLY + LATE, codes[0].shape[1]
    return pl.pallas_call(
        functools.partial(finish_kernel, norm=norm),
        grid_spec=pltpu.PrefetchScalarGridSpec(
            num_scalar_prefetch=1, grid=(4,), in_specs=[WHOLE] * 9,
            out_specs=[pl.BlockSpec((per, LEVELS, cols), lambda s, m: (0, 0, m[0] ^ s)),
                       pl.BlockSpec((per,), lambda s, m: (0,))],
            scratch_shapes=[pltpu.VMEM((8, LANES), F32)]),
        out_shape=[jax.ShapeDtypeStruct((per, LEVELS, 4 * cols), BF),
                   jax.ShapeDtypeStruct((per,), F32)],
        compiler_params=PARAMS, name="finish",
    )(meta, *codes, everyone)


def in_vmem(x):
    return pltpu.with_memory_space_constraint(x, pltpu.VMEM)


def in_hbm(x):
    return pltpu.with_memory_space_constraint(x, pltpu.HBM)


def exchange(part):
    moved = [part[0]]
    for i in range(1, 4):
        moved.append(in_vmem(lax.ppermute(part[i], TRC, [(j, j ^ i) for j in range(4)])))
    return moved


def per_device(tracers_src, layer_dp, cut_frac, level_bounds):
    total_cols = layer_dp.shape[1] * lax.axis_size(COLS_TRC)
    norm = 1.0 / (total_cols * layer_dp.shape[0])
    copies = lax.axis_size(COLS)
    tr = in_hbm(tracers_src.reshape(4, EARLY + LATE, *tracers_src.shape[1:]))
    head = remap_early(tr, in_hbm(layer_dp), in_hbm(cut_frac), in_hbm(level_bounds), total_cols)
    early = exchange(head[:4])
    tail = remap_late(head[4], head[5], head[6:], total_cols, copies)
    everyone = lax.all_to_all(tail[4].reshape(4 * copies, 1, LANES), COLS_TRC, 0, 0, tiled=True)
    late = exchange(tail[:4])
    everyone = in_vmem(everyone.reshape(4 * copies, LANES))
    meta = lax.axis_index(TRC).astype(I32).reshape(1)
    codes = [x for pair in zip(early, late) for x in pair]
    result, burden = finish(meta, codes, everyone, norm)
    return (result, burden)


def solution(mesh):
    split = Mesh(
        mesh.devices.reshape(4, 4, 2, 2, 2), ("cols_0", "cols_1", "cols_2", "trc_0", "trc_1")
    )
    return jax.shard_map(
        per_device,
        mesh=split,
        in_specs=(
            P(None, None, COLS_TRC),
            P(None, COLS_TRC),
            P(None, COLS_TRC),
            P(None, None, COLS_TRC),
        ),
        out_specs=(P(TRC, None, COLS), P(TRC)),
        check_vma=False,
    )
```

```python
import functools
import jax
import jax.numpy as jnp
from jax import lax
from jax.experimental import pallas as pl
from jax.experimental.pallas import tpu as pltpu
from jax.sharding import Mesh
from jax.sharding import PartitionSpec as P

TRC = ("trc_0", "trc_1")
COLS = ("cols_0", "cols_1", "cols_2")
COLS_TRC = ("cols_0", "cols_1", "cols_2", "trc_0", "trc_1")
F32, BF, I32, I16 = jnp.float32, jnp.bfloat16, jnp.int32, jnp.int16
LANES, TILES, OUT = 128, 16, 9
LAYERS, LEVELS, EXTRA = 127, 72, 8
EARLY, LATE = 6, 1

SUBLANE_GATHER = lax.GatherDimensionNumbers(
    offset_dims=(), collapsed_slice_dims=(0,), start_index_map=(0,),
    operand_batching_dims=(1,), start_indices_batching_dims=(1,))


def pick(x, index):
    return lax.gather(x, index[..., None], SUBLANE_GATHER, slice_sizes=(1, 1),
                      mode=lax.GatherScatterMode.PROMISE_IN_BOUNDS)


def tile(x, v):
    return x[8 * v:8 * v + 8]


def row_in_tile():
    return lax.broadcasted_iota(I32, (8, LANES), 0)


def cumulate(tri, mass):
    hi = mass.astype(BF)
    mid = (mass - hi.astype(F32)).astype(BF)
    return jnp.dot(tri[...], jnp.concatenate([hi, mid], axis=0), preferred_element_type=F32)


def edge_differences(cum, extra, cb, idx_s, over_s, one_s, two_s, four_s):
    n = len(cum)
    row8 = row_in_tile()
    y = [[None] * 15 for _ in range(n)]
    z = [[None] * 15 for _ in range(n)]
    w = [[None] * 13 for _ in range(n)]
    edge = [[None] * OUT for _ in range(n)]
    roll = [[None] * OUT for _ in range(n)]
    diff = [[None] * OUT for _ in range(n)]
    point = [tile(cum[i], 0) + extra(i, 0) for i in range(n)]
    for v in range(15):
        ix = idx_s[cb, 8 * v:8 * v + 8, :]
        over = over_s[cb, 8 * v:8 * v + 8, :] != 0
        for i in range(n):
            nxt = tile(cum[i], v + 1) + extra(i, v + 1)
            y[i][v] = jnp.where(over, pick(nxt, ix), pick(point[i], ix))
            point[i] = nxt
        a = v - 1
        if a >= 0:
            m = one_s[cb, 8 * a:8 * a + 8, :] != 0
            for i in range(n):
                z[i][a] = jnp.where(m, y[i][a + 1], y[i][a])
        if v == 14:
            for i in range(n):
                z[i][14] = y[i][14]
        for b in ([v - 3] if v < 14 else [11, 12]):
            if b < 0:
                continue
            m = two_s[cb, 8 * b:8 * b + 8, :] != 0
            for i in range(n):
                w[i][b] = jnp.where(m, z[i][b + 2], z[i][b])
            o = b - 4
            if o < 0:
                continue
            m = four_s[cb, 8 * o:8 * o + 8, :] != 0
            for i in range(n):
                edge[i][o] = jnp.where(m, w[i][o + 4], w[i][o])
                roll[i][o] = pltpu.roll(edge[i][o], 7, 0)
                if o > 0:
                    diff[i][o - 1] = jnp.where(row8 == 7, roll[i][o], roll[i][o - 1]) - edge[i][o - 1]
    for i in range(n):
        total = jnp.broadcast_to(cum[i][LAYERS:LAYERS + 1], (8, LANES))
        diff[i][OUT - 1] = jnp.where(row8 == 7, total, roll[i][OUT - 1]) - edge[i][OUT - 1]
    return diff


def prepare(dp_ref, cf_ref, lb_ref, tri, idx_s, over_s, one_s, two_s, four_s, dp_s, psi_s, inv_s, dbuf, fbuf):
    rr = lax.broadcasted_iota(I32, (LANES, 2 * LANES), 0)
    cc = lax.broadcasted_iota(I32, (LANES, 2 * LANES), 1) & (LANES - 1)
    tri[...] = (cc < rr).astype(F32).astype(BF)
    row8 = row_in_tile()
    zero_i, zero_f = jnp.zeros((8, LANES), I32), jnp.zeros((8, LANES), F32)
    for cb in range(dp_s.shape[0]):
        dbuf[cb, 0:8, :] = zero_i
        fbuf[cb, 0:8, :] = zero_f
        at = slice(cb * LANES, (cb + 1) * LANES)
        d = lb_ref[0, :, at] - lax.broadcasted_iota(I32, (LEVELS, LANES), 0)
        high, low = d >> 3, d & 7
        f = jnp.concatenate([jnp.zeros((1, LANES), F32), cf_ref[:, at]], axis=0)
        for v in range(TILES):
            dv, fv = zero_i, zero_f
            for h in range(7):
                if 0 <= v - h < OUT:
                    m = tile(high, v - h) == h
                    dv = jnp.where(m, tile(low, v - h), dv)
                    fv = jnp.where(m, tile(f, v - h), fv)
            dbuf[cb, 8 + 8 * v:16 + 8 * v, :] = dv
            fbuf[cb, 8 + 8 * v:16 + 8 * v, :] = fv
            t = row8 + dv
            idx_s[cb, 8 * v:8 * v + 8, :] = t & 7
            over_s[cb, 8 * v:8 * v + 8, :] = t >> 3
        for v in range(14):
            bit = zero_i
            for h in (0, 2, 4, 6):
                if 0 <= v - h < OUT:
                    bit = jnp.where(tile(high, v - h) == h + 1, 1, bit)
            one_s[cb, 8 * v:8 * v + 8, :] = bit
        for v in range(13):
            bit = zero_i
            for h in (0, 4):
                if 0 <= v - h < OUT:
                    bit = jnp.where((tile(high, v - h) >> 1) == (h >> 1) + 1, 1, bit)
            two_s[cb, 8 * v:8 * v + 8, :] = bit
        four_s[cb] = high >> 2
        phi = jnp.zeros((LANES, LANES), F32)
        for k in range(8):
            phi = phi + jnp.where(dbuf[cb, 8 - k:136 - k, :] == k, fbuf[cb, 8 - k:136 - k, :], 0.0)
        dp = jnp.concatenate([dp_ref[:, at], jnp.zeros((1, LANES), F32)], axis=0)
        psi = phi * dp
        dp_s[cb] = dp
        psi_s[cb] = psi
        (thick,) = edge_differences(
            [cumulate(tri, dp)], lambda i, v: tile(psi, v), cb, idx_s, over_s, one_s, two_s, four_s)
        for o in range(OUT):
            inv_s[cb, 8 * o:8 * o + 8, :] = 1.0 / thick[o]


def half_step(r, pair, load, outs, row, tabs, extra_s, part, top_s, total_cols):
    tri, idx_s, over_s, one_s, two_s, four_s, dp_s, psi_s, inv_s = tabs
    blocks = dp_s.shape[0]
    start = (lax.axis_index(COLS) * lax.axis_size(TRC) + lax.axis_index(TRC)) * blocks * LANES
    before, after = [None] * 2, [None] * 2
    for cb in range(blocks):
        at = slice(cb * LANES, (cb + 1) * LANES)
        position = start + cb * LANES + lax.broadcasted_iota(I32, (1, LANES), 1)
        area = 1.0 + 2.0 * position.astype(F32) / total_cols
        mass = []
        for i in range(2):
            t = jnp.concatenate([load(i, at).astype(F32), jnp.zeros((1, LANES), F32)], axis=0)
            mass.append(t * dp_s[cb])
            extra_s[cb, i] = t * psi_s[cb]
        both = cumulate(tri, jnp.concatenate(mass, axis=1))
        cum = [both[:, :LANES], both[:, LANES:]]
        diff = edge_differences(
            cum, lambda i, v: extra_s[cb, i, 8 * v:8 * v + 8, :], cb, idx_s, over_s, one_s, two_s, four_s)
        for i in range(2):
            kept = [jnp.maximum(x, 0.0) for x in diff[i]]
            mean = [kept[o] * inv_s[cb, 8 * o:8 * o + 8, :] for o in range(OUT)]
            sums, top = kept[0], mean[0]
            for o in range(1, OUT):
                sums, top = sums + kept[o], jnp.maximum(top, mean[o])
            top = jnp.max(top, axis=0, keepdims=True)
            step = jnp.ceil(jnp.log2(jnp.maximum(top, 1e-33)) * 256.0)
            scale = 65534.0 / jnp.exp2(step * (1.0 / 256.0))
            code = jnp.concatenate([(x * scale + 0.5).astype(I32) for x in mean], axis=0)
            outs[i][pl.ds(pl.multiple_of(row * LEVELS, 8), LEVELS), at] = code.astype(I16)
            top_s[i, cb, pl.ds(row, 1), :] = step
            last, area_sum = cum[i][LAYERS:LAYERS + 1] * area, sums * area
            before[i] = last if cb == 0 else before[i] + last
            after[i] = area_sum if cb == 0 else after[i] + area_sum
    for i in range(2):
        part[r, pair + i:pair + i + 1, :] = before[i]
        part[r, 4 + pair + i:5 + pair + i, :] = jnp.sum(after[i], axis=0, keepdims=True)


def write_tops(size, outs, top_s):
    for i in range(2):
        tops = jnp.concatenate([top_s[i, c] for c in range(top_s.shape[1])], axis=1)
        outs[i][size * LEVELS:size * LEVELS + EXTRA, :] = tops.astype(I32).astype(I16)


def early_kernel(total_cols, tr_hbm, dp_ref, cf_ref, lb_ref, *refs):
    outs, part, near_ref, far_ref, tabs = refs[:2], refs[2], refs[3], refs[4], refs[5:14]
    dbuf, fbuf, held, sems, extra_s, top_s = refs[14:]
    me = lax.axis_index(TRC)
    near = (me >> 1) * 2
    far = 2 - near
    odd = me & 1
    copies = [
        pltpu.make_async_copy(
            tr_hbm.at[pl.ds(far, 2), r], held.at[r] if r < EARLY else far_ref.at[r - EARLY], sems.at[r])
        for r in range(EARLY + LATE)]
    rest = pltpu.make_async_copy(tr_hbm.at[pl.ds(near, 2)], near_ref, sems.at[EARLY + LATE])
    for c in copies[:2]:
        c.start()
    prepare(dp_ref, cf_ref, lb_ref, *tabs, dbuf, fbuf)
    for c in copies[2:]:
        c.start()
    rest.start()

    def steps(g, carry):
        for h in range(2):
            r = 2 * g + h
            pltpu.make_async_copy(tr_hbm.at[pl.ds(far, 2), r], held.at[r], sems.at[r]).wait()
        for h in range(2):
            r = 2 * g + h
            half_step(r, 2, lambda i, at: held[r, odd ^ i, :, at], outs, r, tabs, extra_s.at[h], part, top_s, total_cols)
        return carry

    lax.fori_loop(0, EARLY // 2, steps, 0)
    write_tops(EARLY, outs, top_s)
    for c in copies[EARLY:]:
        c.wait()
    rest.wait()


def late_kernel(total_cols, early_part, near_ref, far_ref, *refs):
    tabs, near_outs, far_outs, sum_ref = refs[:9], refs[9:11], refs[11:13], refs[13]
    extra_s, top_near, top_far, part, fin_s = refs[14:]
    me = lax.axis_index(TRC)
    odd = me & 1
    per = EARLY + LATE

    def near_step(r, h):
        half_step(r, 0, lambda i, at: near_ref[odd ^ i, r, :, at], near_outs, r, tabs,
                  extra_s.at[h], part, top_near, total_cols)

    def steps(g, carry):
        for h in range(2):
            near_step(2 * g + h, h)
        return carry

    lax.fori_loop(0, per // 2, steps, 0)
    near_step(per - 1, 0)
    half_step(EARLY, 2, lambda i, at: far_ref[0, odd ^ i, :, at], far_outs, 0, tabs,
              extra_s.at[1], part, top_far, total_cols)
    write_tops(LATE, far_outs, top_far)
    write_tops(per, near_outs, top_near)
    lane = lax.broadcasted_iota(I32, (8, LANES), 1)
    theirs = (lax.broadcasted_iota(I32, (8, LANES), 0) & 2) != 0
    acc = jnp.zeros((8, LANES), F32)
    for r in range(per):
        p = jnp.where(theirs, early_part[r], part[r]) if r < EARLY else part[r]
        acc = jnp.where(lane == r, jnp.sum(p, axis=1, keepdims=True), acc)
    fin_s[...] = acc
    before = jnp.concatenate([fin_s[pl.ds(me ^ t, 1), :] for t in range(4)], axis=0)
    after = jnp.concatenate([fin_s[pl.ds(4 + (me ^ t), 1), :] for t in range(4)], axis=0)
    lane = lax.broadcasted_iota(I32, (4, LANES), 1)
    both = jnp.where(lane < 64, before, pltpu.roll(after, 64, 1))
    for k in range(sum_ref.shape[0]):
        sum_ref[k] = both


WHOLE = pl.BlockSpec(memory_space=pltpu.VMEM)
PARAMS = pltpu.CompilerParams(vmem_limit_bytes=20 * 2**20)


def cost(size):
    return pl.CostEstimate(flops=size * 1_000_000_000, bytes_accessed=size * 500_000, transcendentals=0)


def profiles(size, cols):
    return [pltpu.VMEM((size * LEVELS + EXTRA, cols), I16)] * 2


def remap_early(tr, dp, cf, lb, total_cols):
    cols = tr.shape[3]
    nb = cols // LANES
    per = EARLY + LATE
    square = (nb, LANES, LANES)
    outs = profiles(EARLY, cols) + [
        pltpu.VMEM((EARLY, 8, LANES), F32),
        pltpu.VMEM((2, per, LAYERS, cols), BF),
        pltpu.VMEM((LATE, 2, LAYERS, cols), BF),
        pltpu.VMEM((LANES, 2 * LANES), BF),
        pltpu.VMEM(square, I32), pltpu.VMEM(square, I32), pltpu.VMEM((nb, 8 * 14, LANES), I32),
        pltpu.VMEM((nb, 8 * 13, LANES), I32), pltpu.VMEM((nb, LEVELS, LANES), I32),
        pltpu.VMEM(square, F32), pltpu.VMEM(square, F32), pltpu.VMEM((nb, LEVELS, LANES), F32),
    ]
    return pl.pallas_call(
        functools.partial(early_kernel, total_cols), grid=(1,),
        in_specs=[
            pl.BlockSpec(memory_space=pltpu.HBM),
            pl.BlockSpec((LAYERS, cols), lambda r: (0, 0)),
            pl.BlockSpec((LEVELS - 1, cols), lambda r: (0, 0)),
            pl.BlockSpec((1, LEVELS, cols), lambda r: (0, 0, 0)),
        ],
        out_specs=[WHOLE] * len(outs), out_shape=outs,
        scratch_shapes=[
            pltpu.VMEM((nb, 136, LANES), I32), pltpu.VMEM((nb, 136, LANES), F32),
            pltpu.VMEM((EARLY, 2, LAYERS, cols), BF), pltpu.SemaphoreType.DMA((per + 1,)),
            pltpu.VMEM((2, nb, 2, LANES, LANES), F32), pltpu.VMEM((2, nb, 8, LANES), F32),
        ],
        compiler_params=PARAMS, cost_estimate=cost(EARLY), name="remap_early",
    )(tr, dp, cf, lb)


def remap_late(part, near, far, tabs, total_cols, copies):
    cols = near.shape[3]
    nb = cols // LANES
    per = EARLY + LATE
    outs = profiles(per, cols) + profiles(LATE, cols) + [pltpu.VMEM((copies, 4, LANES), F32)]
    return pl.pallas_call(
        functools.partial(late_kernel, total_cols), grid=(1,),
        in_specs=[WHOLE] * 12, out_specs=[WHOLE] * len(outs), out_shape=outs,
        scratch_shapes=[
            pltpu.VMEM((2, nb, 2, LANES, LANES), F32), pltpu.VMEM((2, nb, 8, LANES), F32),
            pltpu.VMEM((2, nb, 8, LANES), F32), pltpu.VMEM((per, 8, LANES), F32), pltpu.VMEM((8, LANES), F32),
        ],
        compiler_params=PARAMS, cost_estimate=cost(per + LATE), name="remap_late",
    )(part, near, far, *tabs)


def finish_kernel(*refs, norm):
    near0, near1, early2, early3, late2, late3, all_ref, out_hbm, burden_ref, buf, sems = refs
    per = EARLY + LATE
    me = lax.axis_index(TRC)
    cols = near0.shape[1]
    burden = jnp.sum(all_ref[...], axis=0, keepdims=True) * norm
    burden_ref[...] = burden[0, :per]
    ratio = burden / pltpu.roll(burden, 64, 1) * (1.0 / 65534.0)
    groups = (((near0, per),), ((near1, per),), ((early2, EARLY), (late2, LATE)), ((early3, EARLY), (late3, LATE)))
    tops = [[(ref, k, jnp.exp2(ref[size * LEVELS:size * LEVELS + EXTRA, :].astype(F32) * (1.0 / 256.0))[k:k + 1])
             for ref, size in parts for k in range(size)] for parts in groups]
    copies = []
    for r in range(per):
        for i in range(4):
            ref, k, top = tops[i][r]
            at = pl.ds(pl.multiple_of((me ^ i) * cols, cols), cols)
            code = ref[k * LEVELS:(k + 1) * LEVELS, :].astype(I32) & 65535
            buf[r, :, at] = (code.astype(F32) * (top * ratio[0:1, r:r + 1])).astype(BF)
        copies.append(pltpu.make_async_copy(buf.at[r], out_hbm.at[r], sems.at[r]))
        copies[-1].start()
    for c in copies:
        c.wait()


def finish(codes, everyone, norm):
    per, cols = EARLY + LATE, codes[0].shape[1]
    return pl.pallas_call(
        functools.partial(finish_kernel, norm=norm), grid=(1,),
        in_specs=[WHOLE] * 7,
        out_specs=[pl.BlockSpec(memory_space=pltpu.HBM), pl.BlockSpec((per,), lambda s: (0,))],
        scratch_shapes=[pltpu.VMEM((per, LEVELS, 4 * cols), BF), pltpu.SemaphoreType.DMA((per,))],
        out_shape=[jax.ShapeDtypeStruct((per, LEVELS, 4 * cols), BF),
                   jax.ShapeDtypeStruct((per,), F32)],
        compiler_params=PARAMS, name="finish",
    )(*codes, everyone)


def in_vmem(x):
    return pltpu.with_memory_space_constraint(x, pltpu.VMEM)


def in_hbm(x):
    return pltpu.with_memory_space_constraint(x, pltpu.HBM)


def swap(x, i):
    return in_vmem(lax.ppermute(x, TRC, [(j, j ^ i) for j in range(4)]))


def per_device(tracers_src, layer_dp, cut_frac, level_bounds):
    total_cols = layer_dp.shape[1] * lax.axis_size(COLS_TRC)
    norm = 1.0 / (total_cols * layer_dp.shape[0])
    copies = lax.axis_size(COLS)
    tr = in_hbm(tracers_src.reshape(4, EARLY + LATE, *tracers_src.shape[1:]))
    head = remap_early(tr, in_hbm(layer_dp), in_hbm(cut_frac), in_hbm(level_bounds), total_cols)
    early = [swap(head[i], 2 + i) for i in range(2)]
    tail = remap_late(head[2], head[3], head[4], head[5:], total_cols, copies)
    everyone = lax.all_to_all(tail[4].reshape(4 * copies, 1, LANES), COLS_TRC, 0, 0, tiled=True)
    near = [tail[0], swap(tail[1], 1)]
    late = [swap(tail[2 + i], 2 + i) for i in range(2)]
    everyone = in_vmem(everyone.reshape(4 * copies, LANES))
    return tuple(finish(near + early + late, everyone, norm))


def solution(mesh):
    split = Mesh(
        mesh.devices.reshape(4, 4, 2, 2, 2), ("cols_0", "cols_1", "cols_2", "trc_0", "trc_1")
    )
    return jax.shard_map(
        per_device,
        mesh=split,
        in_specs=(
            P(None, None, COLS_TRC),
            P(None, COLS_TRC),
            P(None, COLS_TRC),
            P(None, None, COLS_TRC),
        ),
        out_specs=(P(TRC, None, COLS), P(TRC)),
        check_vma=False,
    )
```

```python
import functools
import jax
import jax.numpy as jnp
from jax import lax
from jax.experimental import pallas as pl
from jax.experimental.pallas import tpu as pltpu
from jax.sharding import Mesh
from jax.sharding import PartitionSpec as P

TRC = ("trc_0", "trc_1")
COLS = ("cols_0", "cols_1", "cols_2")
COLS_TRC = ("cols_0", "cols_1", "cols_2", "trc_0", "trc_1")
F32, BF, I32, I16 = jnp.float32, jnp.bfloat16, jnp.int32, jnp.int16
LANES, TILES, OUT = 128, 16, 9
LAYERS, LEVELS, EXTRA = 127, 72, 8
EARLY, LATE = 6, 1

SUBLANE_GATHER = lax.GatherDimensionNumbers(
    offset_dims=(), collapsed_slice_dims=(0,), start_index_map=(0,),
    operand_batching_dims=(1,), start_indices_batching_dims=(1,))


def pick(x, index):
    return lax.gather(x, index[..., None], SUBLANE_GATHER, slice_sizes=(1, 1),
                      mode=lax.GatherScatterMode.PROMISE_IN_BOUNDS)


def tile(x, v):
    return x[8 * v:8 * v + 8]


def row_in_tile():
    return lax.broadcasted_iota(I32, (8, LANES), 0)


def cumulate(tri, mass):
    hi = mass.astype(BF)
    mid = (mass - hi.astype(F32)).astype(BF)
    return jnp.dot(tri[...], jnp.concatenate([hi, mid], axis=0), preferred_element_type=F32)


def edge_differences(cum, extra, cb, idx_s, over_s, one_s, two_s, four_s):
    n = len(cum)
    row8 = row_in_tile()
    y = [[None] * 15 for _ in range(n)]
    z = [[None] * 15 for _ in range(n)]
    w = [[None] * 13 for _ in range(n)]
    edge = [[None] * OUT for _ in range(n)]
    roll = [[None] * OUT for _ in range(n)]
    diff = [[None] * OUT for _ in range(n)]
    point = [tile(cum[i], 0) + extra(i, 0) for i in range(n)]
    for v in range(15):
        ix = idx_s[cb, 8 * v:8 * v + 8, :]
        over = over_s[cb, 8 * v:8 * v + 8, :] != 0
        for i in range(n):
            nxt = tile(cum[i], v + 1) + extra(i, v + 1)
            y[i][v] = jnp.where(over, pick(nxt, ix), pick(point[i], ix))
            point[i] = nxt
        a = v - 1
        if a >= 0:
            m = one_s[cb, 8 * a:8 * a + 8, :] != 0
            for i in range(n):
                z[i][a] = jnp.where(m, y[i][a + 1], y[i][a])
        if v == 14:
            for i in range(n):
                z[i][14] = y[i][14]
        for b in ([v - 3] if v < 14 else [11, 12]):
            if b < 0:
                continue
            m = two_s[cb, 8 * b:8 * b + 8, :] != 0
            for i in range(n):
                w[i][b] = jnp.where(m, z[i][b + 2], z[i][b])
            o = b - 4
            if o < 0:
                continue
            m = four_s[cb, 8 * o:8 * o + 8, :] != 0
            for i in range(n):
                edge[i][o] = jnp.where(m, w[i][o + 4], w[i][o])
                roll[i][o] = pltpu.roll(edge[i][o], 7, 0)
                if o > 0:
                    diff[i][o - 1] = jnp.where(row8 == 7, roll[i][o], roll[i][o - 1]) - edge[i][o - 1]
    for i in range(n):
        total = jnp.broadcast_to(cum[i][LAYERS:LAYERS + 1], (8, LANES))
        diff[i][OUT - 1] = jnp.where(row8 == 7, total, roll[i][OUT - 1]) - edge[i][OUT - 1]
    return diff


def prepare(dp_ref, cf_ref, lb_ref, tri, idx_s, over_s, one_s, two_s, four_s, dp_s, psi_s, inv_s, dbuf, fbuf):
    rr = lax.broadcasted_iota(I32, (LANES, 2 * LANES), 0)
    cc = lax.broadcasted_iota(I32, (LANES, 2 * LANES), 1) & (LANES - 1)
    tri[...] = (cc < rr).astype(F32).astype(BF)
    row8 = row_in_tile()
    zero_i, zero_f = jnp.zeros((8, LANES), I32), jnp.zeros((8, LANES), F32)
    for cb in range(dp_s.shape[0]):
        dbuf[cb, 0:8, :] = zero_i
        fbuf[cb, 0:8, :] = zero_f
        at = slice(cb * LANES, (cb + 1) * LANES)
        d = lb_ref[0, :, at] - lax.broadcasted_iota(I32, (LEVELS, LANES), 0)
        high, low = d >> 3, d & 7
        f = jnp.concatenate([jnp.zeros((1, LANES), F32), cf_ref[:, at]], axis=0)
        for v in range(TILES):
            dv, fv = zero_i, zero_f
            for h in range(7):
                if 0 <= v - h < OUT:
                    m = tile(high, v - h) == h
                    dv = jnp.where(m, tile(low, v - h), dv)
                    fv = jnp.where(m, tile(f, v - h), fv)
            dbuf[cb, 8 + 8 * v:16 + 8 * v, :] = dv
            fbuf[cb, 8 + 8 * v:16 + 8 * v, :] = fv
            t = row8 + dv
            idx_s[cb, 8 * v:8 * v + 8, :] = t & 7
            over_s[cb, 8 * v:8 * v + 8, :] = t >> 3
        for v in range(14):
            bit = zero_i
            for h in (0, 2, 4, 6):
                if 0 <= v - h < OUT:
                    bit = jnp.where(tile(high, v - h) == h + 1, 1, bit)
            one_s[cb, 8 * v:8 * v + 8, :] = bit
        for v in range(13):
            bit = zero_i
            for h in (0, 4):
                if 0 <= v - h < OUT:
                    bit = jnp.where((tile(high, v - h) >> 1) == (h >> 1) + 1, 1, bit)
            two_s[cb, 8 * v:8 * v + 8, :] = bit
        four_s[cb] = high >> 2
        phi = jnp.zeros((LANES, LANES), F32)
        for k in range(8):
            phi = phi + jnp.where(dbuf[cb, 8 - k:136 - k, :] == k, fbuf[cb, 8 - k:136 - k, :], 0.0)
        dp = jnp.concatenate([dp_ref[:, at], jnp.zeros((1, LANES), F32)], axis=0)
        psi = phi * dp
        dp_s[cb] = dp
        psi_s[cb] = psi
        (thick,) = edge_differences(
            [cumulate(tri, dp)], lambda i, v: tile(psi, v), cb, idx_s, over_s, one_s, two_s, four_s)
        for o in range(OUT):
            inv_s[cb, 8 * o:8 * o + 8, :] = 1.0 / thick[o]


def encode(outs, row, top_s):
    def sink(i, cb, at, mean):
        top = mean[0]
        for o in range(1, OUT):
            top = jnp.maximum(top, mean[o])
        step, scale = unit(jnp.max(top, axis=0, keepdims=True))
        code = jnp.concatenate([(x * scale + 0.5).astype(I32) for x in mean], axis=0)
        outs[i][pl.ds(pl.multiple_of(row * LEVELS, 8), LEVELS), at] = code.astype(I16)
        top_s[i, cb, pl.ds(row, 1), :] = step

    return sink


def unit(top):
    step = jnp.ceil(jnp.log2(jnp.maximum(top, 1e-33)) * 256.0)
    return step, 65534.0 / jnp.exp2(step * (1.0 / 256.0))


def half_steps(jobs, tabs, extra_s, part, total_cols):
    tri, idx_s, over_s, one_s, two_s, four_s, dp_s, psi_s, inv_s = tabs
    blocks = dp_s.shape[0]
    start = (lax.axis_index(COLS) * lax.axis_size(TRC) + lax.axis_index(TRC)) * blocks * LANES
    before, after = {}, {}
    for cb in range(blocks):
        at = slice(cb * LANES, (cb + 1) * LANES)
        position = start + cb * LANES + lax.broadcasted_iota(I32, (1, LANES), 1)
        area = 1.0 + 2.0 * position.astype(F32) / total_cols
        for h, (_, _, load, sink) in enumerate(jobs):
            mass = []
            for i in range(2):
                t = jnp.concatenate([load(i, at).astype(F32), jnp.zeros((1, LANES), F32)], axis=0)
                mass.append(t * dp_s[cb])
                extra_s[h, cb, i] = t * psi_s[cb]
            both = cumulate(tri, jnp.concatenate(mass, axis=1))
            cum = [both[:, :LANES], both[:, LANES:]]
            diff = edge_differences(
                cum, lambda i, v: extra_s[h, cb, i, 8 * v:8 * v + 8, :], cb, idx_s, over_s, one_s, two_s, four_s)
            for i in range(2):
                kept = [jnp.maximum(x, 0.0) for x in diff[i]]
                sums = kept[0]
                for o in range(1, OUT):
                    sums = sums + kept[o]
                sink(i, cb, at, [kept[o] * inv_s[cb, 8 * o:8 * o + 8, :] for o in range(OUT)])
                last, area_sum = cum[i][LAYERS:LAYERS + 1] * area, sums * area
                before[h, i] = last if cb == 0 else before[h, i] + last
                after[h, i] = area_sum if cb == 0 else after[h, i] + area_sum
    for h, (r, pair, _, _) in enumerate(jobs):
        for i in range(2):
            part[r, pair + i:pair + i + 1, :] = before[h, i]
            part[r, 4 + pair + i:5 + pair + i, :] = jnp.sum(after[h, i], axis=0, keepdims=True)


def write_tops(size, outs, top_s):
    for i in range(2):
        if outs[i] is None:
            continue
        tops = jnp.concatenate([top_s[i, c] for c in range(top_s.shape[1])], axis=1)
        outs[i][size * LEVELS:size * LEVELS + EXTRA, :] = tops.astype(I32).astype(I16)


def early_kernel(total_cols, tr_hbm, dp_ref, cf_ref, lb_ref, *refs):
    result, part, near_ref, far_ref, tabs = refs[:2], refs[2], refs[3], refs[4], refs[5:14]
    dbuf, fbuf, held, sems, extra_s, top_s, out_a, out_b, out_sems = refs[14:]
    outs = (out_a, out_b)
    me = lax.axis_index(TRC)
    near = (me >> 1) * 2
    far = 2 - near
    odd = me & 1
    copies = [
        pltpu.make_async_copy(
            tr_hbm.at[pl.ds(far, 2), r], held.at[r] if r < EARLY else far_ref.at[r - EARLY], sems.at[r])
        for r in range(EARLY + LATE)]
    rest = pltpu.make_async_copy(tr_hbm.at[pl.ds(near, 2)], near_ref, sems.at[EARLY + LATE])
    for c in copies[:2]:
        c.start()
    prepare(dp_ref, cf_ref, lb_ref, *tabs, dbuf, fbuf)
    for c in copies[2:]:
        c.start()
    rest.start()

    def written(g):
        rows = pl.ds(pl.multiple_of(2 * g * LEVELS, 16), 2 * LEVELS)
        return [
            pltpu.make_async_copy(outs[i].at[rows, :], result[i].at[rows, :], out_sems.at[2 * g + i]) for i in range(2)]

    def steps(g, carry):
        for h in range(2):
            r = 2 * g + h
            pltpu.make_async_copy(tr_hbm.at[pl.ds(far, 2), r], held.at[r], sems.at[r]).wait()
        half_steps(
            [(2 * g + h, 2, lambda i, at, h=h: held[2 * g + h, odd ^ i, :, at], encode(outs, 2 * g + h, top_s))
             for h in range(2)], tabs, extra_s, part, total_cols)
        for c in written(g):
            c.start()
        return carry

    lax.fori_loop(0, EARLY // 2, steps, 0)
    write_tops(EARLY, outs, top_s)
    last = [
        pltpu.make_async_copy(
            outs[i].at[EARLY * LEVELS:EARLY * LEVELS + EXTRA, :], result[i].at[EARLY * LEVELS:EARLY * LEVELS + EXTRA, :],
            out_sems.at[EARLY + i])
        for i in range(2)]
    for c in last:
        c.start()
    for g in range(EARLY // 2):
        for c in written(g):
            c.wait()
    for c in last:
        c.wait()
    for c in copies[EARLY:]:
        c.wait()
    rest.wait()


def late_kernel(total_cols, early_part, near_ref, far_ref, *refs):
    tabs, near_outs, far_outs, sum_ref = refs[:9], refs[9:11], refs[11:13], refs[13]
    extra_s, top_near, top_far, part, fin_s = refs[14:]
    me = lax.axis_index(TRC)
    odd = me & 1
    per = EARLY + LATE

    def near_job(r):
        code = encode((None, near_outs[1]), r, top_near)

        def sink(i, cb, at, mean):
            if i == 0:
                near_outs[0][r, :, at] = jnp.concatenate(mean, axis=0)
            else:
                code(i, cb, at, mean)

        return (r, 0, lambda i, at: near_ref[odd ^ i, r, :, at], sink)

    def steps(g, carry):
        half_steps([near_job(2 * g), near_job(2 * g + 1)], tabs, extra_s, part, total_cols)
        return carry

    lax.fori_loop(0, per // 2, steps, 0)
    far_job = (EARLY, 2, lambda i, at: far_ref[0, odd ^ i, :, at], encode(far_outs, 0, top_far))
    half_steps([near_job(per - 1), far_job], tabs, extra_s, part, total_cols)
    write_tops(LATE, far_outs, top_far)
    write_tops(per, (None, near_outs[1]), top_near)
    lane = lax.broadcasted_iota(I32, (8, LANES), 1)
    theirs = (lax.broadcasted_iota(I32, (8, LANES), 0) & 2) != 0
    acc = jnp.zeros((8, LANES), F32)
    for r in range(per):
        p = jnp.where(theirs, early_part[r], part[r]) if r < EARLY else part[r]
        acc = jnp.where(lane == r, jnp.sum(p, axis=1, keepdims=True), acc)
    fin_s[...] = acc
    before = jnp.concatenate([fin_s[pl.ds(me ^ t, 1), :] for t in range(4)], axis=0)
    after = jnp.concatenate([fin_s[pl.ds(4 + (me ^ t), 1), :] for t in range(4)], axis=0)
    lane = lax.broadcasted_iota(I32, (4, LANES), 1)
    both = jnp.where(lane < 64, before, pltpu.roll(after, 64, 1))
    for k in range(sum_ref.shape[0]):
        sum_ref[k] = both


WHOLE = pl.BlockSpec(memory_space=pltpu.VMEM)
PARAMS = pltpu.CompilerParams(vmem_limit_bytes=20 * 2**20)


def cost(size):
    return pl.CostEstimate(flops=size * 1_000_000_000, bytes_accessed=size * 500_000, transcendentals=0)


def profiles(size, cols):
    return [pltpu.VMEM((size * LEVELS + EXTRA, cols), I16)] * 2


def remap_early(tr, dp, cf, lb, total_cols):
    cols = tr.shape[3]
    nb = cols // LANES
    per = EARLY + LATE
    square = (nb, LANES, LANES)
    outs = [jax.ShapeDtypeStruct((EARLY * LEVELS + EXTRA, cols), I16)] * 2 + [
        pltpu.VMEM((EARLY, 8, LANES), F32),
        pltpu.VMEM((2, per, LAYERS, cols), BF),
        pltpu.VMEM((LATE, 2, LAYERS, cols), BF),
        pltpu.VMEM((LANES, 2 * LANES), BF),
        pltpu.VMEM(square, I32), pltpu.VMEM(square, I32), pltpu.VMEM((nb, 8 * 14, LANES), I32),
        pltpu.VMEM((nb, 8 * 13, LANES), I32), pltpu.VMEM((nb, LEVELS, LANES), I32),
        pltpu.VMEM(square, F32), pltpu.VMEM(square, F32), pltpu.VMEM((nb, LEVELS, LANES), F32),
    ]
    return pl.pallas_call(
        functools.partial(early_kernel, total_cols), grid=(1,),
        in_specs=[
            pl.BlockSpec(memory_space=pltpu.HBM),
            pl.BlockSpec((LAYERS, cols), lambda r: (0, 0)),
            pl.BlockSpec((LEVELS - 1, cols), lambda r: (0, 0)),
            pl.BlockSpec((1, LEVELS, cols), lambda r: (0, 0, 0)),
        ],
        out_specs=[pl.BlockSpec(memory_space=pltpu.HBM)] * 2 + [WHOLE] * (len(outs) - 2), out_shape=outs,
        scratch_shapes=[
            pltpu.VMEM((nb, 136, LANES), I32), pltpu.VMEM((nb, 136, LANES), F32),
            pltpu.VMEM((EARLY, 2, LAYERS, cols), BF), pltpu.SemaphoreType.DMA((per + 1,)),
            pltpu.VMEM((2, nb, 2, LANES, LANES), F32), pltpu.VMEM((2, nb, 8, LANES), F32),
        ] + profiles(EARLY, cols) + [pltpu.SemaphoreType.DMA((EARLY + 2,))],
        compiler_params=PARAMS, cost_estimate=cost(EARLY), name="remap_early",
    )(tr, dp, cf, lb)


def remap_late(part, near, far, tabs, total_cols, copies):
    cols = near.shape[3]
    nb = cols // LANES
    per = EARLY + LATE
    outs = [pltpu.VMEM((per, LEVELS, cols), F32), profiles(per, cols)[0]] + profiles(LATE, cols)
    outs += [jax.ShapeDtypeStruct((copies, 4, LANES), F32)]
    return pl.pallas_call(
        functools.partial(late_kernel, total_cols), grid=(1,),
        in_specs=[WHOLE] * 12,
        out_specs=[WHOLE] * 4 + [pl.BlockSpec((copies, 4, LANES), lambda g: (0, 0, 0))], out_shape=outs,
        scratch_shapes=[
            pltpu.VMEM((2, nb, 2, LANES, LANES), F32), pltpu.VMEM((2, nb, 8, LANES), F32),
            pltpu.VMEM((2, nb, 8, LANES), F32), pltpu.VMEM((per, 8, LANES), F32), pltpu.VMEM((8, LANES), F32),
        ],
        compiler_params=PARAMS, cost_estimate=cost(per + LATE), name="remap_late",
    )(part, near, far, *tabs)


def finish_kernel(*refs, norm):
    near0, near1, early2, early3, late2, late3, all_ref, out_hbm, burden_ref, buf, sems = refs
    per = EARLY + LATE
    me = lax.axis_index(TRC)
    cols = near1.shape[1]
    burden = jnp.sum(all_ref[...], axis=0, keepdims=True) * norm
    burden_ref[...] = burden[0, :per]
    plain = burden / pltpu.roll(burden, 64, 1)
    ratio = plain * (1.0 / 65534.0)
    groups = (((near1, per),), ((early2, EARLY), (late2, LATE)), ((early3, EARLY), (late3, LATE)))
    tops = [[(ref, k, jnp.exp2(ref[size * LEVELS:size * LEVELS + EXTRA, :].astype(F32) * (1.0 / 256.0))[k:k + 1])
             for ref, size in parts for k in range(size)] for parts in groups]
    copies = []
    for r in range(per):
        own = pl.ds(pl.multiple_of(me * cols, cols), cols)
        buf[r, :, own] = (near0[r] * plain[0:1, r:r + 1]).astype(BF)
        for i in range(1, 4):
            ref, k, top = tops[i - 1][r]
            at = pl.ds(pl.multiple_of((me ^ i) * cols, cols), cols)
            code = ref[k * LEVELS:(k + 1) * LEVELS, :].astype(I32) & 65535
            buf[r, :, at] = (code.astype(F32) * (top * ratio[0:1, r:r + 1])).astype(BF)
        copies.append(pltpu.make_async_copy(buf.at[r], out_hbm.at[r], sems.at[r]))
        copies[-1].start()
    for c in copies:
        c.wait()


def finish(codes, everyone, norm):
    per, cols = EARLY + LATE, codes[1].shape[1]
    return pl.pallas_call(
        functools.partial(finish_kernel, norm=norm), grid=(1,),
        in_specs=[WHOLE] * 7,
        out_specs=[pl.BlockSpec(memory_space=pltpu.HBM), pl.BlockSpec((per,), lambda s: (0,))],
        scratch_shapes=[pltpu.VMEM((per, LEVELS, 4 * cols), BF), pltpu.SemaphoreType.DMA((per,))],
        out_shape=[jax.ShapeDtypeStruct((per, LEVELS, 4 * cols), BF),
                   jax.ShapeDtypeStruct((per,), F32)],
        compiler_params=PARAMS, name="finish",
    )(*codes, everyone)


def in_vmem(x):
    return pltpu.with_memory_space_constraint(x, pltpu.VMEM)


def in_hbm(x):
    return pltpu.with_memory_space_constraint(x, pltpu.HBM)


def swap(x, i):
    return in_vmem(lax.ppermute(x, TRC, [(j, j ^ i) for j in range(4)]))


def per_device(tracers_src, layer_dp, cut_frac, level_bounds):
    total_cols = layer_dp.shape[1] * lax.axis_size(COLS_TRC)
    norm = 1.0 / (total_cols * layer_dp.shape[0])
    copies = lax.axis_size(COLS)
    tr = in_hbm(tracers_src.reshape(4, EARLY + LATE, *tracers_src.shape[1:]))
    head = remap_early(tr, in_hbm(layer_dp), in_hbm(cut_frac), in_hbm(level_bounds), total_cols)
    early = [swap(head[i], 2 + i) for i in range(2)]
    tail = remap_late(head[2], head[3], head[4], head[5:], total_cols, copies)
    everyone = lax.all_to_all(tail[4].reshape(4 * copies, 1, LANES), COLS_TRC, 0, 0, tiled=True)
    near = [tail[0], swap(tail[1], 1)]
    late = [swap(tail[2 + i], 2 + i) for i in range(2)]
    everyone = in_vmem(everyone.reshape(4 * copies, LANES))
    return tuple(finish(near + early + late, everyone, norm))


def solution(mesh):
    split = Mesh(
        mesh.devices.reshape(4, 4, 2, 2, 2), ("cols_0", "cols_1", "cols_2", "trc_0", "trc_1")
    )
    return jax.shard_map(
        per_device,
        mesh=split,
        in_specs=(
            P(None, None, COLS_TRC),
            P(None, COLS_TRC),
            P(None, COLS_TRC),
            P(None, None, COLS_TRC),
        ),
        out_specs=(P(TRC, None, COLS), P(TRC)),
        check_vma=False,
    )
```

```python
import functools
import jax
import jax.numpy as jnp
from jax import lax
from jax.experimental import pallas as pl
from jax.experimental.pallas import tpu as pltpu
from jax.sharding import Mesh
from jax.sharding import PartitionSpec as P

TRC = ("trc_0", "trc_1")
COLS = ("cols_0", "cols_1", "cols_2")
COLS_TRC = ("cols_0", "cols_1", "cols_2", "trc_0", "trc_1")
F32, BF, I32, I16 = jnp.float32, jnp.bfloat16, jnp.int32, jnp.int16
LANES, TILES, OUT = 128, 16, 9
LAYERS, LEVELS, EXTRA = 127, 72, 8
EARLY, LATE, KEPT = 6, 1, 5

SUBLANE_GATHER = lax.GatherDimensionNumbers(
    offset_dims=(), collapsed_slice_dims=(0,), start_index_map=(0,),
    operand_batching_dims=(1,), start_indices_batching_dims=(1,))


def pick(x, index):
    return lax.gather(x, index[..., None], SUBLANE_GATHER, slice_sizes=(1, 1),
                      mode=lax.GatherScatterMode.PROMISE_IN_BOUNDS)


def tile(x, v):
    return x[8 * v:8 * v + 8]


def row_in_tile():
    return lax.broadcasted_iota(I32, (8, LANES), 0)


def cumulate(tri, mass):
    hi = mass.astype(BF)
    mid = (mass - hi.astype(F32)).astype(BF)
    return jnp.dot(tri[...], jnp.concatenate([hi, mid], axis=0), preferred_element_type=F32)


def edge_differences(cum, extra, cb, idx_s, over_s, one_s, two_s, four_s):
    n = len(cum)
    row8 = row_in_tile()
    y = [[None] * 15 for _ in range(n)]
    z = [[None] * 15 for _ in range(n)]
    w = [[None] * 13 for _ in range(n)]
    edge = [[None] * OUT for _ in range(n)]
    roll = [[None] * OUT for _ in range(n)]
    diff = [[None] * OUT for _ in range(n)]
    point = [tile(cum[i], 0) + extra(i, 0) for i in range(n)]
    for v in range(15):
        ix = idx_s[cb, 8 * v:8 * v + 8, :]
        over = over_s[cb, 8 * v:8 * v + 8, :] != 0
        for i in range(n):
            nxt = tile(cum[i], v + 1) + extra(i, v + 1)
            y[i][v] = jnp.where(over, pick(nxt, ix), pick(point[i], ix))
            point[i] = nxt
        a = v - 1
        if a >= 0:
            m = one_s[cb, 8 * a:8 * a + 8, :] != 0
            for i in range(n):
                z[i][a] = jnp.where(m, y[i][a + 1], y[i][a])
        if v == 14:
            for i in range(n):
                z[i][14] = y[i][14]
        for b in ([v - 3] if v < 14 else [11, 12]):
            if b < 0:
                continue
            m = two_s[cb, 8 * b:8 * b + 8, :] != 0
            for i in range(n):
                w[i][b] = jnp.where(m, z[i][b + 2], z[i][b])
            o = b - 4
            if o < 0:
                continue
            m = four_s[cb, 8 * o:8 * o + 8, :] != 0
            for i in range(n):
                edge[i][o] = jnp.where(m, w[i][o + 4], w[i][o])
                roll[i][o] = pltpu.roll(edge[i][o], 7, 0)
                if o > 0:
                    diff[i][o - 1] = jnp.where(row8 == 7, roll[i][o], roll[i][o - 1]) - edge[i][o - 1]
    for i in range(n):
        total = jnp.broadcast_to(cum[i][LAYERS:LAYERS + 1], (8, LANES))
        diff[i][OUT - 1] = jnp.where(row8 == 7, total, roll[i][OUT - 1]) - edge[i][OUT - 1]
    return diff


def prepare(dp_ref, cf_ref, lb_ref, tri, idx_s, over_s, one_s, two_s, four_s, dp_s, psi_s, inv_s, dbuf, fbuf):
    rr = lax.broadcasted_iota(I32, (LANES, 2 * LANES), 0)
    cc = lax.broadcasted_iota(I32, (LANES, 2 * LANES), 1) & (LANES - 1)
    tri[...] = (cc < rr).astype(F32).astype(BF)
    row8 = row_in_tile()
    zero_i, zero_f = jnp.zeros((8, LANES), I32), jnp.zeros((8, LANES), F32)
    for cb in range(dp_s.shape[0]):
        dbuf[cb, 0:8, :] = zero_i
        fbuf[cb, 0:8, :] = zero_f
        at = slice(cb * LANES, (cb + 1) * LANES)
        d = lb_ref[0, :, at] - lax.broadcasted_iota(I32, (LEVELS, LANES), 0)
        high, low = d >> 3, d & 7
        f = jnp.concatenate([jnp.zeros((1, LANES), F32), cf_ref[:, at]], axis=0)
        for v in range(TILES):
            dv, fv = zero_i, zero_f
            for h in range(7):
                if 0 <= v - h < OUT:
                    m = tile(high, v - h) == h
                    dv = jnp.where(m, tile(low, v - h), dv)
                    fv = jnp.where(m, tile(f, v - h), fv)
            dbuf[cb, 8 + 8 * v:16 + 8 * v, :] = dv
            fbuf[cb, 8 + 8 * v:16 + 8 * v, :] = fv
            t = row8 + dv
            idx_s[cb, 8 * v:8 * v + 8, :] = t & 7
            over_s[cb, 8 * v:8 * v + 8, :] = t >> 3
        for v in range(14):
            bit = zero_i
            for h in (0, 2, 4, 6):
                if 0 <= v - h < OUT:
                    bit = jnp.where(tile(high, v - h) == h + 1, 1, bit)
            one_s[cb, 8 * v:8 * v + 8, :] = bit
        for v in range(13):
            bit = zero_i
            for h in (0, 4):
                if 0 <= v - h < OUT:
                    bit = jnp.where((tile(high, v - h) >> 1) == (h >> 1) + 1, 1, bit)
            two_s[cb, 8 * v:8 * v + 8, :] = bit
        four_s[cb] = high >> 2
        phi = jnp.zeros((LANES, LANES), F32)
        for k in range(8):
            phi = phi + jnp.where(dbuf[cb, 8 - k:136 - k, :] == k, fbuf[cb, 8 - k:136 - k, :], 0.0)
        dp = jnp.concatenate([dp_ref[:, at], jnp.zeros((1, LANES), F32)], axis=0)
        psi = phi * dp
        dp_s[cb] = dp
        psi_s[cb] = psi
        (thick,) = edge_differences(
            [cumulate(tri, dp)], lambda i, v: tile(psi, v), cb, idx_s, over_s, one_s, two_s, four_s)
        for o in range(OUT):
            inv_s[cb, 8 * o:8 * o + 8, :] = 1.0 / thick[o]


def encode(outs, row, top_s):
    def sink(i, cb, at, mean):
        top = mean[0]
        for o in range(1, OUT):
            top = jnp.maximum(top, mean[o])
        step, scale = unit(jnp.max(top, axis=0, keepdims=True))
        code = jnp.concatenate([(x * scale + 0.5).astype(I32) for x in mean], axis=0)
        outs[i][pl.ds(pl.multiple_of(row * LEVELS, 8), LEVELS), at] = code.astype(I16)
        top_s[i, cb, pl.ds(row, 1), :] = step

    return sink


def unit(top):
    step = jnp.ceil(jnp.log2(jnp.maximum(top, 1e-33)) * 256.0)
    return step, 65534.0 / jnp.exp2(step * (1.0 / 256.0))


def half_steps(jobs, tabs, extra_s, part, total_cols):
    tri, idx_s, over_s, one_s, two_s, four_s, dp_s, psi_s, inv_s = tabs
    blocks = dp_s.shape[0]
    start = (lax.axis_index(COLS) * lax.axis_size(TRC) + lax.axis_index(TRC)) * blocks * LANES
    before, after = {}, {}
    for cb in range(blocks):
        at = slice(cb * LANES, (cb + 1) * LANES)
        position = start + cb * LANES + lax.broadcasted_iota(I32, (1, LANES), 1)
        area = 1.0 + 2.0 * position.astype(F32) / total_cols
        for h, (_, _, load, sink) in enumerate(jobs):
            mass = []
            for i in range(2):
                t = jnp.concatenate([load(i, at).astype(F32), jnp.zeros((1, LANES), F32)], axis=0)
                mass.append(t * dp_s[cb])
                extra_s[h, cb, i] = t * psi_s[cb]
            both = cumulate(tri, jnp.concatenate(mass, axis=1))
            cum = [both[:, :LANES], both[:, LANES:]]
            diff = edge_differences(
                cum, lambda i, v: extra_s[h, cb, i, 8 * v:8 * v + 8, :], cb, idx_s, over_s, one_s, two_s, four_s)
            for i in range(2):
                kept = [jnp.maximum(x, 0.0) for x in diff[i]]
                sums = kept[0]
                for o in range(1, OUT):
                    sums = sums + kept[o]
                sink(i, cb, at, [kept[o] * inv_s[cb, 8 * o:8 * o + 8, :] for o in range(OUT)])
                last, area_sum = cum[i][LAYERS:LAYERS + 1] * area, sums * area
                before[h, i] = last if cb == 0 else before[h, i] + last
                after[h, i] = area_sum if cb == 0 else after[h, i] + area_sum
    for h, (r, pair, _, _) in enumerate(jobs):
        for i in range(2):
            part[r, pair + i:pair + i + 1, :] = before[h, i]
            part[r, 4 + pair + i:5 + pair + i, :] = jnp.sum(after[h, i], axis=0, keepdims=True)


def write_tops(size, outs, top_s):
    for i in range(2):
        if outs[i] is None:
            continue
        tops = jnp.concatenate([top_s[i, c] for c in range(top_s.shape[1])], axis=1)
        outs[i][size * LEVELS:size * LEVELS + EXTRA, :] = tops.astype(I32).astype(I16)


def early_kernel(total_cols, tr_hbm, dp_ref, cf_ref, lb_ref, *refs):
    result, part, near_ref, far_ref, tabs, spare = refs[:2], refs[2], refs[3], refs[4], refs[5:14], refs[14]
    dbuf, fbuf, held, sems, extra_s, top_s, out_a, out_b, out_sems = refs[15:]
    outs = (out_a, out_b)
    me = lax.axis_index(TRC)
    near = (me >> 1) * 2
    far = 2 - near
    odd = me & 1
    copies = [
        pltpu.make_async_copy(
            tr_hbm.at[pl.ds(far, 2), r], held.at[r] if r < EARLY else far_ref.at[r - EARLY], sems.at[r])
        for r in range(EARLY + LATE)]
    rest = pltpu.make_async_copy(tr_hbm.at[pl.ds(near, 2)], near_ref, sems.at[EARLY + LATE])
    for c in copies[:2]:
        c.start()
    prepare(dp_ref, cf_ref, lb_ref, *tabs, dbuf, fbuf)
    for c in copies[2:]:
        c.start()
    rest.start()

    def written(g):
        rows = pl.ds(pl.multiple_of(2 * g * LEVELS, 16), 2 * LEVELS)
        return [
            pltpu.make_async_copy(outs[i].at[rows, :], result[i].at[rows, :], out_sems.at[2 * g + i]) for i in range(2)]

    def steps(g, carry):
        for h in range(2):
            r = 2 * g + h
            pltpu.make_async_copy(tr_hbm.at[pl.ds(far, 2), r], held.at[r], sems.at[r]).wait()
        half_steps(
            [(2 * g + h, 2, lambda i, at, h=h: held[2 * g + h, odd ^ i, :, at], encode(outs, 2 * g + h, top_s))
             for h in range(2)], tabs, extra_s, part, total_cols)
        both = written(g)
        both[0].start()
        pl.when(g < EARLY // 2 - 1)(both[1].start)
        return carry

    lax.fori_loop(0, EARLY // 2, steps, 0)
    write_tops(EARLY, outs, top_s)
    ends = ((EARLY * LEVELS, EARLY * LEVELS, EXTRA), (EARLY * LEVELS, KEPT * LEVELS, EXTRA))
    ends += ((2 * (EARLY // 2 - 1) * LEVELS, 2 * (EARLY // 2 - 1) * LEVELS, LEVELS),)
    last = [
        pltpu.make_async_copy(
            outs[min(i, 1)].at[a:a + n, :], result[min(i, 1)].at[b:b + n, :], out_sems.at[EARLY + i])
        for i, (a, b, n) in enumerate(ends)]
    for c in last:
        c.start()
    spare[...] = out_b[KEPT * LEVELS:EARLY * LEVELS, :]
    for g in range(EARLY // 2):
        for c in written(g)[:2 if g < EARLY // 2 - 1 else 1]:
            c.wait()
    for c in last:
        c.wait()
    for c in copies[EARLY:]:
        c.wait()
    rest.wait()


def late_kernel(total_cols, early_part, near_ref, far_ref, spare, *refs):
    tabs, near_outs, far_outs, sum_ref = refs[:9], refs[9:11], refs[11:13], refs[13]
    extra_s, top_near, top_far, part, fin_s = refs[14:]
    me = lax.axis_index(TRC)
    odd = me & 1
    per = EARLY + LATE

    def near_job(r):
        code = encode((None, near_outs[1]), r, top_near)

        def sink(i, cb, at, mean):
            if i == 0:
                near_outs[0][r, :, at] = jnp.concatenate(mean, axis=0)
            else:
                code(i, cb, at, mean)

        return (r, 0, lambda i, at: near_ref[odd ^ i, r, :, at], sink)

    def steps(g, carry):
        half_steps([near_job(2 * g), near_job(2 * g + 1)], tabs, extra_s, part, total_cols)
        return carry

    lax.fori_loop(0, per // 2, steps, 0)
    far_job = (EARLY, 2, lambda i, at: far_ref[0, odd ^ i, :, at], encode(far_outs, 0, top_far))
    half_steps([near_job(per - 1), far_job], tabs, extra_s, part, total_cols)
    write_tops(LATE, far_outs, top_far)
    far_outs[1][LATE * LEVELS + EXTRA:, :] = spare[...]
    write_tops(per, (None, near_outs[1]), top_near)
    lane = lax.broadcasted_iota(I32, (8, LANES), 1)
    theirs = (lax.broadcasted_iota(I32, (8, LANES), 0) & 2) != 0
    acc = jnp.zeros((8, LANES), F32)
    for r in range(per):
        p = jnp.where(theirs, early_part[r], part[r]) if r < EARLY else part[r]
        acc = jnp.where(lane == r, jnp.sum(p, axis=1, keepdims=True), acc)
    fin_s[...] = acc
    before = jnp.concatenate([fin_s[pl.ds(me ^ t, 1), :] for t in range(4)], axis=0)
    after = jnp.concatenate([fin_s[pl.ds(4 + (me ^ t), 1), :] for t in range(4)], axis=0)
    lane = lax.broadcasted_iota(I32, (4, LANES), 1)
    both = jnp.where(lane < 64, before, pltpu.roll(after, 64, 1))
    for k in range(sum_ref.shape[0]):
        sum_ref[k] = both


WHOLE = pl.BlockSpec(memory_space=pltpu.VMEM)
PARAMS = pltpu.CompilerParams(vmem_limit_bytes=20 * 2**20)


def cost(size):
    return pl.CostEstimate(flops=size * 1_000_000_000, bytes_accessed=size * 500_000, transcendentals=0)


def profiles(size, cols):
    return [pltpu.VMEM((size * LEVELS + EXTRA, cols), I16)] * 2


def remap_early(tr, dp, cf, lb, total_cols):
    cols = tr.shape[3]
    nb = cols // LANES
    per = EARLY + LATE
    square = (nb, LANES, LANES)
    outs = [jax.ShapeDtypeStruct((n * LEVELS + EXTRA, cols), I16) for n in (EARLY, KEPT)] + [
        pltpu.VMEM((EARLY, 8, LANES), F32),
        pltpu.VMEM((2, per, LAYERS, cols), BF),
        pltpu.VMEM((LATE, 2, LAYERS, cols), BF),
        pltpu.VMEM((LANES, 2 * LANES), BF),
        pltpu.VMEM(square, I32), pltpu.VMEM(square, I32), pltpu.VMEM((nb, 8 * 14, LANES), I32),
        pltpu.VMEM((nb, 8 * 13, LANES), I32), pltpu.VMEM((nb, LEVELS, LANES), I32),
        pltpu.VMEM(square, F32), pltpu.VMEM(square, F32), pltpu.VMEM((nb, LEVELS, LANES), F32),
        pltpu.VMEM((LEVELS, cols), I16),
    ]
    return pl.pallas_call(
        functools.partial(early_kernel, total_cols), grid=(1,),
        in_specs=[
            pl.BlockSpec(memory_space=pltpu.HBM),
            pl.BlockSpec((LAYERS, cols), lambda r: (0, 0)),
            pl.BlockSpec((LEVELS - 1, cols), lambda r: (0, 0)),
            pl.BlockSpec((1, LEVELS, cols), lambda r: (0, 0, 0)),
        ],
        out_specs=[pl.BlockSpec(memory_space=pltpu.HBM)] * 2 + [WHOLE] * (len(outs) - 2), out_shape=outs,
        scratch_shapes=[
            pltpu.VMEM((nb, 136, LANES), I32), pltpu.VMEM((nb, 136, LANES), F32),
            pltpu.VMEM((EARLY, 2, LAYERS, cols), BF), pltpu.SemaphoreType.DMA((per + 1,)),
            pltpu.VMEM((2, nb, 2, LANES, LANES), F32), pltpu.VMEM((2, nb, 8, LANES), F32),
        ] + profiles(EARLY, cols) + [pltpu.SemaphoreType.DMA((EARLY + 3,))],
        compiler_params=PARAMS, cost_estimate=cost(EARLY), name="remap_early",
    )(tr, dp, cf, lb)


def remap_late(part, near, far, spare, tabs, total_cols, copies):
    cols = near.shape[3]
    nb = cols // LANES
    per = EARLY + LATE
    outs = [pltpu.VMEM((per, LEVELS, cols), F32), profiles(per, cols)[0], profiles(LATE, cols)[0]]
    outs += [pltpu.VMEM(((LATE + 1) * LEVELS + EXTRA, cols), I16)]
    outs += [jax.ShapeDtypeStruct((copies, 4, LANES), F32)]
    return pl.pallas_call(
        functools.partial(late_kernel, total_cols), grid=(1,),
        in_specs=[WHOLE] * 13,
        out_specs=[WHOLE] * 4 + [pl.BlockSpec((copies, 4, LANES), lambda g: (0, 0, 0))], out_shape=outs,
        scratch_shapes=[
            pltpu.VMEM((2, nb, 2, LANES, LANES), F32), pltpu.VMEM((2, nb, 8, LANES), F32),
            pltpu.VMEM((2, nb, 8, LANES), F32), pltpu.VMEM((per, 8, LANES), F32), pltpu.VMEM((8, LANES), F32),
        ],
        compiler_params=PARAMS, cost_estimate=cost(per + LATE), name="remap_late",
    )(part, near, far, spare, *tabs)


def finish_kernel(*refs, norm):
    near0, near1, early2, early3, late2, late3, all_ref, out_hbm, burden_ref, buf, sems = refs
    per = EARLY + LATE
    me = lax.axis_index(TRC)
    cols = near1.shape[1]
    burden = jnp.sum(all_ref[...], axis=0, keepdims=True) * norm
    burden_ref[...] = burden[0, :per]
    plain = burden / pltpu.roll(burden, 64, 1)
    ratio = plain * (1.0 / 65534.0)

    def tops_of(ref, size):
        return jnp.exp2(ref[size * LEVELS:size * LEVELS + EXTRA, :].astype(F32) * (1.0 / 256.0))

    near_top, top2, top3 = tops_of(near1, per), tops_of(early2, EARLY), tops_of(early3, KEPT)
    end2, end3 = tops_of(late2, LATE), tops_of(late3, LATE)
    tops = [[(near1, k * LEVELS, near_top[k:k + 1]) for k in range(per)],
            [(early2, k * LEVELS, top2[k:k + 1]) for k in range(EARLY)] + [(late2, 0, end2[0:1])],
            [(early3, k * LEVELS, top3[k:k + 1]) for k in range(KEPT)]
            + [(late3, LATE * LEVELS + EXTRA, top3[KEPT:EARLY]), (late3, 0, end3[0:1])]]
    copies = []
    for r in range(per):
        own = pl.ds(pl.multiple_of(me * cols, cols), cols)
        buf[r, :, own] = (near0[r] * plain[0:1, r:r + 1]).astype(BF)
        for i in range(1, 4):
            ref, k, top = tops[i - 1][r]
            at = pl.ds(pl.multiple_of((me ^ i) * cols, cols), cols)
            code = ref[k:k + LEVELS, :].astype(I32) & 65535
            buf[r, :, at] = (code.astype(F32) * (top * ratio[0:1, r:r + 1])).astype(BF)
        copies.append(pltpu.make_async_copy(buf.at[r], out_hbm.at[r], sems.at[r]))
        copies[-1].start()
    for c in copies:
        c.wait()


def finish(codes, everyone, norm):
    per, cols = EARLY + LATE, codes[1].shape[1]
    return pl.pallas_call(
        functools.partial(finish_kernel, norm=norm), grid=(1,),
        in_specs=[WHOLE] * 7,
        out_specs=[pl.BlockSpec(memory_space=pltpu.HBM), pl.BlockSpec((per,), lambda s: (0,))],
        scratch_shapes=[pltpu.VMEM((per, LEVELS, 4 * cols), BF), pltpu.SemaphoreType.DMA((per,))],
        out_shape=[jax.ShapeDtypeStruct((per, LEVELS, 4 * cols), BF),
                   jax.ShapeDtypeStruct((per,), F32)],
        compiler_params=PARAMS, name="finish",
    )(*codes, everyone)


def in_vmem(x):
    return pltpu.with_memory_space_constraint(x, pltpu.VMEM)


def in_hbm(x):
    return pltpu.with_memory_space_constraint(x, pltpu.HBM)


def swap(x, i):
    return in_vmem(lax.ppermute(x, TRC, [(j, j ^ i) for j in range(4)]))


def per_device(tracers_src, layer_dp, cut_frac, level_bounds):
    total_cols = layer_dp.shape[1] * lax.axis_size(COLS_TRC)
    norm = 1.0 / (total_cols * layer_dp.shape[0])
    copies = lax.axis_size(COLS)
    tr = in_hbm(tracers_src.reshape(4, EARLY + LATE, *tracers_src.shape[1:]))
    head = remap_early(tr, in_hbm(layer_dp), in_hbm(cut_frac), in_hbm(level_bounds), total_cols)
    early = [swap(head[i], 2 + i) for i in range(2)]
    tail = remap_late(head[2], head[3], head[4], head[14], head[5:14], total_cols, copies)
    everyone = lax.all_to_all(tail[4].reshape(4 * copies, 1, LANES), COLS_TRC, 0, 0, tiled=True)
    near = [tail[0], swap(tail[1], 1)]
    late = [swap(tail[2 + i], 2 + i) for i in range(2)]
    everyone = in_vmem(everyone.reshape(4 * copies, LANES))
    return tuple(finish(near + early + late, everyone, norm))


def solution(mesh):
    split = Mesh(
        mesh.devices.reshape(4, 4, 2, 2, 2), ("cols_0", "cols_1", "cols_2", "trc_0", "trc_1")
    )
    return jax.shard_map(
        per_device,
        mesh=split,
        in_specs=(
            P(None, None, COLS_TRC),
            P(None, COLS_TRC),
            P(None, COLS_TRC),
            P(None, None, COLS_TRC),
        ),
        out_specs=(P(TRC, None, COLS), P(TRC)),
        check_vma=False,
    )
```
